128 devices in a mesh: dp: 4 (over z), seq: 8 (over y_lo, x), tensor: 4 (over y_hi, core).
Axes of the slice: x: 4, y: 4 (y_hi: 2, y_lo: 2; y = y_hi * 2 + y_lo), z: 4, core: 2. Of those that a mesh axis runs over, the one named last changes fastest.
Arguments:
- hidden_in: bfloat16 [65536, 2880], P(('dp', 'seq', 'tensor')), parts along dimension 0, may hold values from -6 to 6
- norm_gain: float32 [2880], replicated, may hold values from 0.5 to 1.5
- conv_weight: float32 [4, 2880], replicated, may hold values from -3 to 3
- w_query: bfloat16 [2880, 2048], P(None, 'tensor'), may hold values from -32 to 32
- w_key: bfloat16 [2880, 512], P(None, 'tensor'), may hold values from -1 to 1
- w_value: bfloat16 [2880, 512], P(None, 'tensor'), may hold values from -0.109375 to 0.109375
- w_out: bfloat16 [2048, 2880], P('tensor'), may hold values from -0.125 to 0.125
- doc_ids: int32 [65536], P(('dp', 'seq')), parts along dimension 0, may hold values from 0 to 63, never falling along the last dimension, each value on 1 to 1024 neighbouring positions
Outputs:
- hidden_out: bfloat16 [65536, 2880], P(('dp', 'seq', 'tensor')), parts along dimension 0
The draws below stay inside these ranges and needn't reach their ends.
There are 4 independent parts, one for each index of `dp`. The reference program is written for one: setup_inputs(seed, part) draws one part's arguments, and reference() takes and returns one part's arrays. A program takes and returns all parts, laid end to end along the dimension named above; an argument that names none is the same for every part. Nothing has to cross between parts.
Inputs may be any that keep to these rules, and one draw needn't show every extreme that they name: `doc_ids`: document numbers never fall along a window's tokens.
All inputs are finite; a program needn't handle non-finite values.
Results may differ from the reference program's by a relative error of at most 0.011.
Values may be sent and summed in bfloat16 or wider, within the bound.
A program may use at most 128 MiB of HBM per device.

```python
import math
import jax
import jax.numpy as jnp
import numpy as np
from jax import lax

D = 2880
HEADS = 32
KV_HEADS = 8
HEAD = 64
KERNEL = 4
WINDOW = 128
QBLOCK = 512
TOKENS = 16384
DOC_MOST = 1024
DOCS = 64


def key_matrix(key):
    scale = 1.0 / math.sqrt(D)
    raw = jax.random.normal(jax.random.fold_in(key, 11), (D, KV_HEADS * HEAD), jnp.float32) * scale
    return jnp.clip(raw, -5.0 * scale, 5.0 * scale)


def draw_w_key(key, part):
    return key_matrix(key).astype(jnp.bfloat16)


def draw_w_query(key, part):
    noise = jax.random.normal(jax.random.fold_in(key, 13), (D, HEADS * HEAD), jnp.float32) * (1.0 / math.sqrt(D))
    return noise.astype(jnp.bfloat16)


def steps_of(rng, shape, pieces, least, high):
    level = 1.0
    for dim, blocks in pieces:
        draws = jax.random.uniform(jax.random.fold_in(jax.random.fold_in(rng, 6), dim), (blocks,), jnp.float32, least / len(pieces), high / len(pieces))
        level = level * jnp.repeat(jnp.exp(draws), shape[dim] // blocks).reshape((-1,) + (1,) * (len(shape) - 1 - dim))
    return level


def length_profile(number_of, total, reach, lean):
    loads = [(1 << 20) // math.isqrt(grade ** lean) + 1 for grade in range(2, number_of + 1)]
    surplus, given = total - reach - (number_of - 1), [1] * (number_of - 1)
    while surplus > 0:
        movable = [i for i in range(number_of - 1) if given[i] < reach]
        pool, left = sum([loads[i] for i in movable]), surplus
        for i in movable:
            addition = min(reach - given[i], max(1, left * loads[i] // pool), surplus)
            given[i] = given[i] + addition
            surplus = surplus - addition
    return np.array([reach] + given)


def uneven_parts(own_key, amount, total, reach, slope):
    if amount == 2:
        one = jax.random.randint(own_key, (), max(1, total - reach), min(reach, total - 1) + 1)
        return jnp.stack([one, total - one])
    lengths = jnp.asarray(length_profile(amount, total, reach, slope), jnp.int32)
    pairs = (amount - 1) // 2
    donor, sink = lengths[1:1 + 2 * pairs:2], lengths[2:2 + 2 * pairs:2]
    slack = jnp.minimum(donor - 1, reach - sink)
    moved = jax.random.randint(jax.random.fold_in(own_key, 1), (pairs,), 0, 1 << 20) % (slack + 1)
    lengths = lengths.at[1:1 + 2 * pairs:2].set(donor - moved).at[2:2 + 2 * pairs:2].set(sink + moved)
    return lengths[jax.random.permutation(jax.random.fold_in(own_key, 2), amount)]


def normal_values(stream_key, extent, deviation, most, split=(), kind=jnp.bfloat16):
    loudness = steps_of(stream_key, extent, split, -0.22, 0.18) if split else 1.0
    values = jax.random.normal(stream_key, extent, jnp.float32) * deviation * loudness
    return jnp.minimum(jnp.maximum(values, -most), most).astype(kind)


def setup_inputs(seed: int = 0, part: int = 0) -> dict:
    arg_keys = jax.random.split(jax.random.key(seed), 9)
    part_keys = jax.random.split(jax.random.fold_in(arg_keys[8], part), 9)
    return {
        "hidden_in": normal_values(part_keys[0], (TOKENS, D), 1.0, 6.0, ((0, 32),)),
        "norm_gain": jnp.clip(1.0 + 0.1 * jax.random.normal(arg_keys[1], (D,), jnp.float32), 0.5, 1.5),
        "conv_weight": normal_values(arg_keys[2], (KERNEL, D), 0.5, 3.0, (), jnp.float32),
        "w_query": draw_w_query(jax.random.fold_in(arg_keys[8], 71), part),
        "w_key": draw_w_key(jax.random.fold_in(arg_keys[8], 71), part),
        "w_value": normal_values(arg_keys[5], (D, KV_HEADS * HEAD), D ** -0.5, 0.109375, ((1, 4),)),
        "w_out": normal_values(arg_keys[6], (HEADS * HEAD, D), (HEADS * HEAD) ** -0.5, 0.125, ((0, 4),)),
        "doc_ids": jnp.searchsorted(jnp.cumsum(uneven_parts(part_keys[7], DOCS, TOKENS, DOC_MOST, 2)), jnp.arange(TOKENS), side="right").astype(jnp.int32),
    }


eps = 1e-05
rope_base = 150000.0

def rotate(values, positions):
    rows = values.shape[0]
    half = HEAD // 2
    frequency = jnp.exp(jnp.arange(half, dtype=jnp.float32) * (-2.0 * math.log(rope_base) / HEAD))
    angle = positions.astype(jnp.float32)[:, None] * frequency[None, :]
    cosine = jnp.cos(angle)[:, None, :]
    sine = jnp.sin(angle)[:, None, :]
    shaped = values.reshape(rows, -1, HEAD)
    first = shaped[:, :, :half]
    second = shaped[:, :, half:]
    turned = jnp.concatenate([first * cosine - second * sine, second * cosine + first * sine], axis=2)
    return turned.reshape(rows, -1)

def attend(queries, keys, values, query_pos, key_pos, query_doc, key_doc):
    scores = jnp.einsum('qhgd,khd->hgqk', queries.astype(jnp.float32), keys.astype(jnp.float32)) * (1.0 / math.sqrt(HEAD))
    visible = (key_pos[None, :] <= query_pos[:, None]) & (key_pos[None, :] > query_pos[:, None] - WINDOW)
    visible = visible & (key_pos[None, :] >= 0) & (key_doc[None, :] == query_doc[:, None])
    scores = jnp.where(visible[None, None, :, :], scores, -jnp.inf)
    largest = lax.optimization_barrier(jnp.max(scores, axis=3, keepdims=True))
    weights = jnp.exp(scores - largest)
    total = lax.optimization_barrier(jnp.sum(weights, axis=3))
    rounded = weights.astype(jnp.bfloat16)
    summed = jnp.einsum('hgqk,khd->qhgd', rounded.astype(jnp.float32), values.astype(jnp.float32))
    result = summed / jnp.transpose(total, (2, 0, 1))[:, :, :, None]
    return result.reshape(result.shape[0], -1).astype(jnp.bfloat16)

def reference(hidden_in, norm_gain, conv_weight, w_query, w_key, w_value, w_out, doc_ids):
    total_rows = hidden_in.shape[0]
    inputs = hidden_in.astype(jnp.float32)
    mean_square = lax.optimization_barrier(jnp.mean(inputs * inputs, axis=1, keepdims=True))
    normed = (inputs * lax.rsqrt(mean_square + eps) * norm_gain[None, :]).astype(jnp.bfloat16)
    padded = jnp.concatenate([jnp.zeros((KERNEL - 1, D), jnp.float32), normed.astype(jnp.float32)], axis=0)
    convolved = jnp.zeros((total_rows, D), jnp.float32)
    for tap in range(KERNEL):
        convolved = convolved + conv_weight[tap][None, :] * padded[KERNEL - 1 - tap:KERNEL - 1 - tap + total_rows]
    mixed = convolved.astype(jnp.bfloat16)
    positions = jnp.arange(total_rows, dtype=jnp.int32)
    queries = rotate(jnp.dot(mixed, w_query, preferred_element_type=jnp.float32), positions).astype(jnp.bfloat16)
    keys = rotate(jnp.dot(mixed, w_key, preferred_element_type=jnp.float32), positions).astype(jnp.bfloat16)
    values = jnp.dot(mixed, w_value, preferred_element_type=jnp.float32).astype(jnp.bfloat16)
    groups = HEADS // KV_HEADS
    query_four = queries.reshape(total_rows, KV_HEADS, groups, HEAD)
    key_pad = jnp.concatenate([jnp.zeros((WINDOW, KV_HEADS * HEAD), jnp.bfloat16), keys], axis=0).reshape(total_rows + WINDOW, KV_HEADS, HEAD)
    value_pad = jnp.concatenate([jnp.zeros((WINDOW, KV_HEADS * HEAD), jnp.bfloat16), values], axis=0).reshape(total_rows + WINDOW, KV_HEADS, HEAD)
    doc_pad = jnp.concatenate([jnp.full((WINDOW,), -1, jnp.int32), doc_ids.astype(jnp.int32)], axis=0)
    pos_pad = jnp.arange(total_rows + WINDOW, dtype=jnp.int32) - WINDOW

    def one_block(index):
        begin = (index * QBLOCK).astype(jnp.int32)
        block_q = lax.dynamic_slice_in_dim(query_four, begin, QBLOCK, 0)
        block_k = lax.dynamic_slice_in_dim(key_pad, begin, QBLOCK + WINDOW, 0)
        block_v = lax.dynamic_slice_in_dim(value_pad, begin, QBLOCK + WINDOW, 0)
        query_pos = lax.dynamic_slice_in_dim(positions, begin, QBLOCK, 0)
        key_pos = lax.dynamic_slice_in_dim(pos_pad, begin, QBLOCK + WINDOW, 0)
        query_doc = lax.dynamic_slice_in_dim(doc_ids.astype(jnp.int32), begin, QBLOCK, 0)
        key_doc = lax.dynamic_slice_in_dim(doc_pad, begin, QBLOCK + WINDOW, 0)
        return attend(block_q, block_k, block_v, query_pos, key_pos, query_doc, key_doc)
    blocks = lax.map(one_block, jnp.arange(total_rows // QBLOCK, dtype=jnp.int32))
    attended = blocks.reshape(total_rows, HEADS * HEAD)
    projected = jnp.dot(attended, w_out, preferred_element_type=jnp.float32)
    return (inputs + projected).astype(jnp.bfloat16)
```

```python
import math

import jax
import jax.numpy as jnp
import numpy as np
from jax import lax
from jax.experimental import pallas as pl
from jax.experimental.pallas import tpu as pltpu
from jax.sharding import PartitionSpec as P

HEAD = 64
WINDOW = 128
EPS = 1e-05
ROPE_BASE = 150000.0
NEG = -1e30
MESH = pl.DeviceIdType.MESH

D = 2880
ROWS = 512
CHIP = 2 * ROWS
NB = CHIP // WINDOW
HALO = 16
CB = 64
NCB = ROWS // CB
GM = 256
PIECE = D // 8
CHUNKS = 5
A, B, AL, AR, BL, BR, ALL_, BRR = range(8)


def rope_tables():
    half = HEAD // 2
    frequency = np.exp(np.arange(half) * (-2.0 * math.log(ROPE_BASE) / HEAD))
    lanes = np.tile(frequency, 4)
    inner = np.arange(WINDOW)[:, None] * lanes[None, :]
    outer = (np.arange(128) * WINDOW)[:, None] * lanes[None, :]
    return np.stack([np.cos(inner), np.sin(inner), np.cos(outer), np.sin(outer)]).astype(np.float32)


def kernel(
    hid_h, gain_h, conv_h, wq_h, wk_h, wv_h, wo_h, doc_h, rope_h, out_h,
    hid, gain, conv, mixed, w, wo, rope, cosv, sinv, doc, dprev, docx, bias,
    q, kx, vx, tail, halo, att, psend, precv, outv,
    load_sem, wsem_s, wsem_r, mix_s, mix_r, edge_s, edge_r, kv_s, kv_r, part_s, part_r, out_sem,
):
    dp, seq, tensor = lax.axis_index("dp"), lax.axis_index("seq"), lax.axis_index("tensor")
    yh, core = tensor // 2, tensor % 2
    yl, x = seq // 4, seq % 4
    cross = (dp, (1 - yl) * 4 + x, (1 - yh) * 2 + core)
    ylo = (dp, (1 - yl) * 4 + x, tensor)
    right = ((dp, yl * 4 + (x + 1) % 4, tensor), ((dp + 1) % 4, seq, tensor))
    left = ((dp, yl * 4 + (x + 3) % 4, tensor), ((dp + 3) % 4, seq, tensor))
    partner = (dp, seq, yh * 2 + (1 - core))
    place = seq * 2 + yh
    nplace, pplace = (place + 1) % 16, (place + 15) % 16
    next_chip = (dp, nplace // 2, (nplace % 2) * 2 + core)
    prev_chip = (dp, pplace // 2, (pplace % 2) * 2 + core)
    order = seq * 4 + tensor
    norder, porder = (order + 1) % 32, (order + 31) % 32
    next_dev = (dp, norder // 4, norder % 4)
    prev_dev = (dp, porder // 4, porder % 4)
    ring = (x, dp)

    own = pl.multiple_of(core * ROWS, ROWS)
    other = pl.multiple_of((1 - core) * ROWS, ROWS)

    def local(i, src, dst):
        return pltpu.make_async_copy(src, dst, load_sem.at[i])

    doc_rows = pl.ds(pl.multiple_of(yh * 8, 8), 8)
    loads = [
        local(0, hid_h, hid.at[pl.ds(HALO, ROWS)]),
        local(1, gain_h, gain),
        local(2, conv_h, conv),
        local(3, rope_h, rope),
        local(4, doc_h.at[doc_rows], doc),
        local(5, wk_h, w.at[0, 0]),
        local(6, wv_h, w.at[0, 3]),
        local(7, wq_h.at[:, pl.ds(0, 128)], w.at[0, 1]),
        local(8, wq_h.at[:, pl.ds(128, 128)], w.at[0, 2]),
        local(9, wq_h.at[:, pl.ds(256, 128)], w.at[0, 4]),
        local(10, wq_h.at[:, pl.ds(384, 128)], w.at[0, 5]),
        local(11, wo_h, wo.at[pl.ds(0, 512)]),
    ]
    for load in loads:
        load.start()

    barrier = pltpu.get_barrier_semaphore()
    peers = [cross, ylo, *right, *left, partner, next_chip, prev_chip, next_dev, prev_dev]
    for peer in peers:
        pl.semaphore_signal(barrier, inc=1, device_id=peer, device_id_type=MESH)
    pl.semaphore_wait(barrier, len(peers))

    def remote(src, dst, send, recv, device):
        return pltpu.make_async_remote_copy(
            src_ref=src, dst_ref=dst, send_sem=send, recv_sem=recv,
            device_id=device, device_id_type=MESH,
        )

    def piece(s, c, at, l):
        if c < 3:
            start = pl.multiple_of(at * (2 * PIECE) + l * PIECE, 8)
            return w.at[1, s * 3 + c, pl.ds(start, PIECE)]
        start = pl.multiple_of(512 + s * 256 + (c - 3) * 128 + (at * 2 + l) * 16, 16)
        return wo.at[pl.ds(start, 16)]

    def source(s, c, at, l):
        if c < 3:
            rows = pl.ds(pl.multiple_of(at * (2 * PIECE) + l * PIECE, 8), PIECE)
            if c == 0:
                return (wk_h, wv_h)[s].at[rows]
            return wq_h.at[rows, pl.ds(s * 256 + (c - 1) * 128, 128)]
        start = pl.multiple_of(s * 256 + (c - 3) * 128 + (at * 2 + l) * 16, 16)
        return wo_h.at[pl.ds(start, 16)]

    sent = []

    def send(s, c, kind, src, dst, device):
        copy = remote(src, dst, wsem_s.at[s, c, kind], wsem_r.at[s, c, kind], device)
        copy.start()
        sent.append(copy)

    def arrived(s, c, kind, at, l):
        ref = piece(s, c, at, l)
        remote(ref, ref, wsem_s.at[s, c, kind], wsem_r.at[s, c, kind], cross).wait_recv()

    def before(s):
        return (ring[s] + 3) % 4

    def after(s):
        return (ring[s] + 1) % 4

    def over(s):
        return (ring[s] + 2) % 4

    def s0(c):
        for s in range(2):
            arrived(s, c, A, ring[s], yl)
            ref = piece(s, c, ring[s], yl)
            send(s, c, AL, ref, ref, right[s])
            send(s, c, AR, ref, ref, left[s])
            send(s, c, B, ref, ref, ylo)

    def s1(c):
        for s in range(2):
            arrived(s, c, B, ring[s], 1 - yl)
            ref = piece(s, c, ring[s], 1 - yl)
            send(s, c, BR, ref, ref, left[s])
            send(s, c, BL, ref, ref, right[s])
            arrived(s, c, AL, before(s), yl)
            ref = piece(s, c, before(s), yl)
            send(s, c, ALL_, ref, ref, right[s])

    def s2(c):
        for s in range(2):
            arrived(s, c, BR, after(s), 1 - yl)
            ref = piece(s, c, after(s), 1 - yl)
            send(s, c, BRR, ref, ref, left[s])

    def s3(c):
        for s in range(2):
            arrived(s, c, AR, after(s), yl)
            arrived(s, c, BL, before(s), 1 - yl)
            arrived(s, c, ALL_, over(s), yl)
            arrived(s, c, BRR, over(s), 1 - yl)

    edge = [
        remote(hid_h.at[pl.ds(ROWS - HALO, HALO)], hid.at[pl.ds(0, HALO)], edge_s.at[0], edge_r.at[0], next_dev),
        remote(doc_h.at[doc_rows], dprev, edge_s.at[1], edge_r.at[1], next_chip),
    ]
    for copy in edge:
        copy.start()
    for c in range(CHUNKS):
        for s in range(2):
            send(s, c, A, source(s, c, ring[s], 1 - yl), piece(s, c, ring[s], 1 - yl), cross)

    for i in range(3):
        loads[i].wait()

    def norm_conv(b):
        base = pl.multiple_of(b * CB, CB)
        rows = pl.ds(base, CB + HALO)
        total = jnp.zeros((CB + 8, 128), jnp.float32)
        for lane in range(0, D - 64, 128):
            v = hid[rows, lane:lane + 128].astype(jnp.float32)[8:]
            total = total + v * v
        v = hid[rows, D - 64:D].astype(jnp.float32)[8:]
        square = jnp.sum(total, axis=1, keepdims=True) + jnp.sum(v * v, axis=1, keepdims=True)
        scale = lax.rsqrt(square * (1.0 / D) + EPS)
        first = jnp.logical_and(b == 0, order == 0)
        row = lax.broadcasted_iota(jnp.int32, (CB + 8, 1), 0)
        keep = jnp.where(first, 0.0, 1.0)
        scale = jnp.where(row < 8, scale * keep, scale)
        at = pl.multiple_of(own + base, CB)
        for lane in range(0, D, 128):
            width = min(128, D - lane)
            cols = slice(lane, lane + width)
            v = hid[rows, cols].astype(jnp.float32)[8:]
            n = (v * scale * gain[:, cols]).astype(jnp.bfloat16).astype(jnp.float32)
            m = conv[0:1, cols] * n[8:]
            for tap in range(1, 4):
                m = m + conv[tap:tap + 1, cols] * pltpu.roll(n, tap, 0)[8:]
            mixed[pl.ds(at, CB), cols] = m.astype(jnp.bfloat16)

    def mix_copy(b, start):
        rows = pl.ds(pl.multiple_of(start + b * CB, CB), CB)
        return remote(mixed.at[rows], mixed.at[rows], mix_s.at[b], mix_r.at[b], partner)

    def norm_step(b, carry):
        norm_conv(b)
        mix_copy(b, own).start()
        return carry

    lax.fori_loop(1, 4, norm_step, 0)
    s0(0)
    lax.fori_loop(4, 6, norm_step, 0)
    s0(1)
    lax.fori_loop(6, NCB, norm_step, 0)
    edge[0].wait()
    norm_step(0, 0)
    s1(0)
    s0(2)

    loads[3].wait()
    loads[4].wait()
    edge[1].wait()
    lane = lax.broadcasted_iota(jnp.int32, (1, 128), 1)
    sign = jnp.where(lane % 64 < 32, -1.0, 1.0)
    docx[0:1, :] = jnp.where(place == 0, -1.0, dprev[7:8, :].astype(jnp.float32))
    docx[1:9, :] = doc[...].astype(jnp.float32)

    def table_step(b, carry):
        rows = pl.ds(pl.multiple_of(b * WINDOW, WINDOW), WINDOW)
        cb = rope[2, pl.ds(place * NB + b, 1), :]
        sb = rope[3, pl.ds(place * NB + b, 1), :]
        cosv[rows, :] = rope[0] * cb - rope[1] * sb
        sinv[rows, :] = (rope[1] * cb + rope[0] * sb) * sign
        r = lax.broadcasted_iota(jnp.int32, (128, 128), 0)
        c = lax.broadcasted_iota(jnp.int32, (128, 128), 1)
        k0 = docx[pl.ds(b, 1), :]
        k1 = docx[pl.ds(b + 1, 1), :]
        mine = jnp.sum(jnp.where(r == c, k1, 0.0), axis=1, keepdims=True)
        bias[b, :, 0:128] = jnp.where(jnp.logical_and(c > r, k0 == mine), 0.0, NEG)
        bias[b, :, 128:256] = jnp.where(jnp.logical_and(c <= r, k1 == mine), 0.0, NEG)
        return carry

    lax.fori_loop(0, NB, table_step, 0)

    def spread(dst, g, rows, v):
        low = lax.broadcasted_iota(jnp.int32, v.shape, 1) < 64
        turned = pltpu.roll(v, 64, 1)
        dst[g, 0, rows, :] = jnp.where(low, v, 0.0).astype(jnp.bfloat16)
        dst[g, 1, rows, :] = jnp.where(low, 0.0, turned).astype(jnp.bfloat16)
        dst[g, 2, rows, :] = jnp.where(low, turned, 0.0).astype(jnp.bfloat16)
        dst[g, 3, rows, :] = jnp.where(low, 0.0, v).astype(jnp.bfloat16)

    def project(g, start):
        rows = pl.ds(start, GM)
        ext = pl.ds(pl.multiple_of(start + WINDOW, WINDOW), GM)
        weights = jnp.concatenate([w[g, j] for j in range(6)], axis=1)
        p = jnp.dot(mixed[rows, :], weights, preferred_element_type=jnp.float32)
        cosine, sine = cosv[rows, :], sinv[rows, :]
        low = lax.broadcasted_iota(jnp.int32, (GM, 128), 1) % 64 < 32

        def turn(v):
            return v * cosine + jnp.where(low, pltpu.roll(v, 96, 1), pltpu.roll(v, 32, 1)) * sine

        k = turn(p[:, 0:128])
        v = p[:, 384:512]
        spread(kx, g, ext, k)
        spread(vx, g, ext, v)
        tail[g, 0, rows, :] = k.astype(jnp.bfloat16)
        tail[g, 1, rows, :] = v.astype(jnp.bfloat16)
        for i, j in enumerate((1, 2, 4, 5)):
            v = turn(p[:, j * 128:(j + 1) * 128])
            q[g, rows, i * 128:(i + 1) * 128] = (v * 0.125).astype(jnp.bfloat16)

    def project_rows(g, start):
        def step(i, carry):
            project(g, pl.multiple_of(start + i * GM, GM))
            return carry

        lax.fori_loop(0, ROWS // GM, step, 0)

    def kv_copy(g, i):
        return remote(
            tail.at[g, i, pl.ds(CHIP - WINDOW, WINDOW)], halo.at[1 - g, i],
            kv_s.at[g, i], kv_r.at[1 - g, i], next_chip,
        )

    def attend(g, b):
        rows = pl.ds(pl.multiple_of(b * WINDOW, WINDOW), WINDOW)
        keys = pl.ds(pl.multiple_of(b * WINDOW, WINDOW), 2 * WINDOW)
        extra = bias[b]
        extra = jnp.concatenate([extra, extra], axis=0)
        low = lax.broadcasted_iota(jnp.int32, (256, 128), 1) < 64
        for j in range(2):
            cols = j * 256
            both = jnp.concatenate([q[g, rows, cols:cols + 128], q[g, rows, cols + 128:cols + 256]], axis=0)
            k2 = jnp.concatenate([kx[g, 2 * j, keys, :], kx[g, 2 * j + 1, keys, :]], axis=0)
            v2 = jnp.concatenate([vx[g, 2 * j, keys, :], vx[g, 2 * j + 1, keys, :]], axis=0)
            s = lax.dot_general(both, k2, (((1,), (1,)), ((), ())), preferred_element_type=jnp.float32)
            weights, inverse = [], []
            for i in range(2):
                half = s[:, i * 256:(i + 1) * 256] + extra
                e = jnp.exp(half - jnp.max(half, axis=1, keepdims=True))
                inverse.append(1.0 / jnp.sum(e, axis=1, keepdims=True))
                weights.append(e.astype(jnp.bfloat16))
            o = jnp.dot(jnp.concatenate(weights, axis=1), v2, preferred_element_type=jnp.float32)
            o = (o * jnp.where(low, inverse[0], inverse[1])).astype(jnp.bfloat16)
            att[rows, g * 512 + cols:g * 512 + cols + 128] = o[0:128]
            att[rows, g * 512 + cols + 128:g * 512 + cols + 256] = o[128:256]

    def attend_blocks(g, low, high):
        def step(b, carry):
            attend(g, b)
            return carry

        lax.fori_loop(low, high, step, 0)

    def attend_first(g):
        for i in range(2):
            copy = remote(
                halo.at[g, i], halo.at[g, i], kv_s.at[1 - g, i], kv_r.at[g, i], prev_chip
            )
            copy.wait_recv()
        spread(kx, g, pl.ds(0, WINDOW), halo[g, 0].astype(jnp.float32))
        spread(vx, g, pl.ds(0, WINDOW), halo[g, 1].astype(jnp.float32))
        attend(g, 0)

    for i in range(5, 11):
        loads[i].wait()
    project_rows(0, own)
    s1(1)
    s0(3)
    for b in range(NCB):
        mix_copy(b, other).wait_recv()
    project_rows(0, other)
    for i in range(2):
        kv_copy(0, i).start()
    s2(0)
    s1(2)
    s0(4)
    attend_blocks(0, 1, 4)
    s2(1)
    s1(3)
    attend_blocks(0, 4, 6)
    s2(2)
    attend_blocks(0, 6, 8)
    s1(4)
    for c in range(3):
        s3(c)
    project_rows(1, own)
    s2(3)
    project_rows(1, other)
    for i in range(2):
        kv_copy(1, i).start()
    s2(4)
    attend_first(0)
    attend_blocks(1, 1, 8)
    attend_first(1)

    loads[11].wait()
    for c in range(3, 5):
        s3(c)
    OM = 128

    def part_copy(i):
        rows = pl.ds(pl.multiple_of(i * OM, OM), OM)
        return remote(psend.at[rows], precv.at[rows], part_s.at[i], part_r.at[i], partner)

    def out_copy(i):
        rows = pl.ds(pl.multiple_of(i * OM, OM), OM)
        return pltpu.make_async_copy(outv.at[rows], out_h.at[rows], out_sem.at[i])

    def far_step(i, carry):
        p = jnp.dot(
            att[pl.ds(pl.multiple_of(other + i * OM, OM), OM), :], wo[...],
            preferred_element_type=jnp.float32,
        )
        psend[pl.ds(pl.multiple_of(i * OM, OM), OM), :] = p.astype(jnp.bfloat16)
        part_copy(i).start()
        return carry

    def near_step(i, carry):
        rows = pl.ds(pl.multiple_of(i * OM, OM), OM)
        p = jnp.dot(
            att[pl.ds(pl.multiple_of(own + i * OM, OM), OM), :], wo[...],
            preferred_element_type=jnp.float32,
        )
        part_copy(i).wait_recv()
        p = p + precv[rows, :].astype(jnp.float32)
        base = hid[pl.ds(pl.multiple_of(HALO + i * OM, 16), OM), :].astype(jnp.float32)
        outv[rows, :] = (base + p).astype(jnp.bfloat16)
        out_copy(i).start()
        return carry

    lax.fori_loop(0, ROWS // OM, far_step, 0)
    lax.fori_loop(0, ROWS // OM, near_step, 0)

    for i in range(ROWS // OM):
        out_copy(i).wait()
        part_copy(i).wait_send()
    for b in range(NCB):
        mix_copy(b, own).wait_send()
    for g in range(2):
        for i in range(2):
            kv_copy(g, i).wait_send()
    for copy in sent:
        copy.wait_send()


def local(hidden_in, norm_gain, conv_weight, w_query, w_key, w_value, w_out, doc_ids):
    bf16, f32 = jnp.bfloat16, jnp.float32
    vmem, dma = pltpu.VMEM, pltpu.SemaphoreType.DMA
    scratch = [
        vmem((HALO + ROWS, D), bf16),
        vmem((1, D), f32),
        vmem((4, D), f32),
        vmem((CHIP, D), bf16),
        vmem((2, 6, D, 128), bf16),
        vmem((1024, D), bf16),
        vmem((4, 128, 128), f32),
        vmem((CHIP, 128), f32),
        vmem((CHIP, 128), f32),
        vmem((8, 128), jnp.int32),
        vmem((8, 128), jnp.int32),
        vmem((16, 128), f32),
        vmem((NB, 128, 256), f32),
        vmem((2, CHIP, 512), bf16),
        vmem((2, 4, CHIP + WINDOW, 128), bf16),
        vmem((2, 4, CHIP + WINDOW, 128), bf16),
        vmem((2, 2, CHIP, 128), bf16),
        vmem((2, 2, WINDOW, 128), bf16),
        vmem((CHIP, 1024), bf16),
        vmem((ROWS, D), bf16),
        vmem((ROWS, D), bf16),
        vmem((ROWS, D), bf16),
        dma((12,)),
        dma((2, CHUNKS, 8)),
        dma((2, CHUNKS, 8)),
        dma((NCB,)),
        dma((NCB,)),
        dma((2,)),
        dma((2,)),
        dma((2, 2)),
        dma((2, 2)),
        dma((4,)),
        dma((4,)),
        dma((4,)),
    ]
    hbm = pl.BlockSpec(memory_space=pl.ANY)
    return pl.pallas_call(
        kernel,
        out_shape=jax.ShapeDtypeStruct((ROWS, D), bf16),
        in_specs=[hbm] * 9,
        out_specs=hbm,
        scratch_shapes=scratch,
        compiler_params=pltpu.CompilerParams(
            collective_id=0, has_side_effects=True, vmem_limit_bytes=67043328
        ),
        name="attention_block",
    )(
        hidden_in, norm_gain.reshape(1, D), conv_weight, w_query, w_key, w_value, w_out,
        doc_ids.reshape(16, 128), jnp.asarray(rope_tables()),
    )


def solution(mesh):
    in_specs = (
        P(("dp", "seq", "tensor"), None),
        P(),
        P(),
        P(None, "tensor"),
        P(None, "tensor"),
        P(None, "tensor"),
        P("tensor", None),
        P(("dp", "seq")),
    )
    out_specs = P(("dp", "seq", "tensor"), None)
    return jax.shard_map(local, mesh=mesh, in_specs=in_specs, out_specs=out_specs, check_vma=False)
```

```python
import math

import jax
import jax.numpy as jnp
import numpy as np
from jax import lax
from jax.experimental import pallas as pl
from jax.experimental.pallas import tpu as pltpu
from jax.sharding import PartitionSpec as P

HEAD = 64
WINDOW = 128
EPS = 1e-05
ROPE_BASE = 150000.0
NEG = -1e30
MESH = pl.DeviceIdType.MESH

D = 2880
ROWS = 512
CHIP = 2 * ROWS
NB = CHIP // WINDOW
HALO = 16
TB = 256
FC = D // 4
CB = 64
NCB = ROWS // CB
PIECE = D // 8
CHUNKS = 5
SLOTS = (
    ((0, 0),),
    ((0, 1), (1, 0)),
    ((0, 2),),
    ((2, 0), (1, 1)),
    ((0, 3),),
    ((2, 1), (1, 2)),
    ((0, 4),),
    ((2, 2), (1, 3)),
    (),
    ((2, 3),),
    ((1, 4),),
    ((2, 4),),
    (),
    (),
    (),
)
A, B, AL, AR, BL, BR, ALL_, BRR = range(8)


def rope_tables():
    half = HEAD // 2
    frequency = np.exp(np.arange(half) * (-2.0 * math.log(ROPE_BASE) / HEAD))
    lanes = np.tile(frequency, 4)
    inner = np.arange(WINDOW)[:, None] * lanes[None, :]
    outer = (np.arange(128) * WINDOW)[:, None] * lanes[None, :]
    return np.stack([np.cos(inner), np.sin(inner), np.cos(outer), np.sin(outer)]).astype(np.float32)


def kernel(
    hid_h, gain, conv_h, wq_h, wk_h, wv_h, wo_h, doc_h, rope_h, out_h,
    hid, flat, conv, mixed, w, rope, cosv, sinv, doc, dprev, docx, bias,
    q, kx, vx, tail, halo, att, acc, psend, precv,
    load_sem, wsem_s, wsem_r, mix_s, mix_r, edge_s, edge_r, kv_s, kv_r, part_s, part_r, out_sem,
):
    dp, seq, tensor = lax.axis_index("dp"), lax.axis_index("seq"), lax.axis_index("tensor")
    yh, core = tensor // 2, tensor % 2
    yl, x = seq // 4, seq % 4
    cross = (dp, (1 - yl) * 4 + x, (1 - yh) * 2 + core)
    ylo = (dp, (1 - yl) * 4 + x, tensor)
    right = ((dp, yl * 4 + (x + 1) % 4, tensor), ((dp + 1) % 4, seq, tensor))
    left = ((dp, yl * 4 + (x + 3) % 4, tensor), ((dp + 3) % 4, seq, tensor))
    partner = (dp, seq, yh * 2 + (1 - core))
    place = seq * 2 + yh
    nplace, pplace = (place + 1) % 16, (place + 15) % 16
    next_chip = (dp, nplace // 2, (nplace % 2) * 2 + core)
    prev_chip = (dp, pplace // 2, (pplace % 2) * 2 + core)
    order = seq * 4 + tensor
    norder, porder = (order + 1) % 32, (order + 31) % 32
    next_dev = (dp, norder // 4, norder % 4)
    prev_dev = (dp, porder // 4, porder % 4)
    ring = (x, dp)

    own = pl.multiple_of(core * ROWS, ROWS)
    other = pl.multiple_of((1 - core) * ROWS, ROWS)

    def local(i, src, dst):
        return pltpu.make_async_copy(src, dst, load_sem.at[i])

    doc_rows = pl.ds(pl.multiple_of(yh * 8, 8), 8)
    loads = [
        local(0, hid_h, flat),
        local(1, conv_h, conv),
        local(2, rope_h, rope),
        local(3, doc_h.at[doc_rows], doc),
        local(4, wk_h, w.at[0, 0]),
        local(5, wv_h, w.at[0, 5]),
    ]
    for j in range(4):
        cols = pl.ds(j * 128, 128)
        loads.append(local(6 + j, wq_h.at[:, cols], w.at[0, (j % 2) * 5 + 1 + j // 2]))
    for j in range(4):
        cols = pl.ds(j * 128, 128)
        loads.append(local(10 + j, wo_h.at[:, cols], w.at[0, (j % 2) * 5 + 3 + j // 2]))
    for load in loads:
        load.start()

    barrier = pltpu.get_barrier_semaphore()
    peers = [cross, ylo, *right, *left, partner, next_chip, prev_chip, next_dev, prev_dev]
    for peer in peers:
        pl.semaphore_signal(barrier, inc=1, device_id=peer, device_id_type=MESH)
    pl.semaphore_wait(barrier, len(peers))

    def remote(src, dst, send, recv, device):
        return pltpu.make_async_remote_copy(
            src_ref=src, dst_ref=dst, send_sem=send, recv_sem=recv,
            device_id=device, device_id_type=MESH,
        )

    def span(at, l):
        return pl.ds(pl.multiple_of(at * (2 * PIECE) + l * PIECE, 8), PIECE)

    def piece(s, c, at, l):
        return w.at[1, s * CHUNKS + c, span(at, l)]

    def source(s, c, at, l):
        if c == 0:
            return (wk_h, wv_h)[s].at[span(at, l)]
        ref = wq_h if c < 3 else wo_h
        return ref.at[span(at, l), pl.ds((((c - 1) % 2) * 2 + s) * 128, 128)]

    sent = []

    def send(s, c, kind, src, dst, device):
        copy = remote(src, dst, wsem_s.at[s, c, kind], wsem_r.at[s, c, kind], device)
        copy.start()
        sent.append(copy)

    def arrived(s, c, kind, at, l):
        ref = piece(s, c, at, l)
        remote(ref, ref, wsem_s.at[s, c, kind], wsem_r.at[s, c, kind], cross).wait_recv()

    def before(s):
        return (ring[s] + 3) % 4

    def after(s):
        return (ring[s] + 1) % 4

    def over(s):
        return (ring[s] + 2) % 4

    def s0(c):
        for s in range(2):
            arrived(s, c, A, ring[s], yl)
            ref = piece(s, c, ring[s], yl)
            send(s, c, AL, ref, ref, right[s])
            send(s, c, AR, ref, ref, left[s])
            send(s, c, B, ref, ref, ylo)

    def s1(c):
        for s in range(2):
            arrived(s, c, B, ring[s], 1 - yl)
            ref = piece(s, c, ring[s], 1 - yl)
            send(s, c, BR, ref, ref, left[s])
            send(s, c, BL, ref, ref, right[s])
            arrived(s, c, AL, before(s), yl)
            ref = piece(s, c, before(s), yl)
            send(s, c, ALL_, ref, ref, right[s])

    def s2(c):
        for s in range(2):
            arrived(s, c, BR, after(s), 1 - yl)
            ref = piece(s, c, after(s), 1 - yl)
            send(s, c, BRR, ref, ref, left[s])

    def s3(c):
        for s in range(2):
            arrived(s, c, AR, after(s), yl)
            arrived(s, c, BL, before(s), 1 - yl)
            arrived(s, c, ALL_, over(s), yl)
            arrived(s, c, BRR, over(s), 1 - yl)

    stages = (s0, s1, s2)

    def slot(i):
        for stage, c in SLOTS[i]:
            stages[stage](c)

    edge = [
        remote(hid.at[pl.ds(HALO + ROWS - 8, 8)], hid.at[pl.ds(8, 8)], edge_s.at[0], edge_r.at[0], next_dev),
        remote(doc_h.at[doc_rows], dprev, edge_s.at[1], edge_r.at[1], next_chip),
    ]
    for c in range(CHUNKS):
        for s in range(2):
            send(s, c, A, source(s, c, ring[s], 1 - yl), piece(s, c, ring[s], 1 - yl), cross)
    edge[1].start()

    for i in range(2):
        loads[i].wait()
    unit = lax.broadcasted_iota(jnp.int32, (TB, TB), 0) == lax.broadcasted_iota(jnp.int32, (TB, TB), 1)
    unit = jnp.where(unit, 1.0, 0.0).astype(jnp.bfloat16)

    def transpose(i):
        for f in range(0, D, 768):
            rows = slice(f, min(f + 768, D))
            turned = lax.dot_general(
                unit, flat[rows, i * TB:(i + 1) * TB], (((1,), (1,)), ((), ())),
                preferred_element_type=jnp.float32,
            )
            hid[HALO + i * TB:HALO + (i + 1) * TB, rows] = turned.astype(jnp.bfloat16)

    transpose(1)
    transpose(0)
    edge[0].start()

    def norm_conv(b):
        base = pl.multiple_of(b * CB, CB)
        rows = pl.ds(base, CB + HALO)
        total = jnp.zeros((CB + 8, 128), jnp.float32)
        for lane in range(0, D - 64, 128):
            v = hid[rows, lane:lane + 128].astype(jnp.float32)[8:]
            total = total + v * v
        v = hid[rows, D - 64:D].astype(jnp.float32)[8:]
        square = jnp.sum(total, axis=1, keepdims=True) + jnp.sum(v * v, axis=1, keepdims=True)
        scale = lax.rsqrt(square * (1.0 / D) + EPS)
        first = jnp.logical_and(b == 0, order == 0)
        row = lax.broadcasted_iota(jnp.int32, (CB + 8, 1), 0)
        keep = jnp.where(first, 0.0, 1.0)
        scale = jnp.where(row < 8, scale * keep, scale)
        at = pl.multiple_of(own + base, CB)
        for lane in range(0, D, 128):
            width = min(128, D - lane)
            cols = slice(lane, lane + width)
            v = hid[rows, cols].astype(jnp.float32)[8:]
            n = (v * scale * gain[cols].reshape(1, width)).astype(jnp.bfloat16).astype(jnp.float32)
            m = conv[0:1, cols] * n[8:]
            for tap in range(1, 4):
                m = m + conv[tap:tap + 1, cols] * pltpu.roll(n, tap, 0)[8:]
            mixed[pl.ds(at, CB), cols] = m.astype(jnp.bfloat16)

    def mix_copy(b, start):
        rows = pl.ds(pl.multiple_of(start + b * CB, CB), CB)
        return remote(mixed.at[rows], mixed.at[rows], mix_s.at[b], mix_r.at[b], partner)

    def norm_step(b, carry):
        norm_conv(b)
        mix_copy(b, own).start()
        return carry

    lax.fori_loop(1, NCB, norm_step, 0)
    edge[0].wait()
    norm_step(0, 0)
    slot(0)

    loads[2].wait()
    loads[3].wait()
    edge[1].wait()
    lane = lax.broadcasted_iota(jnp.int32, (1, 128), 1)
    sign = jnp.where(lane % 64 < 32, -1.0, 1.0)
    docx[0:1, :] = jnp.where(place == 0, -1.0, dprev[7:8, :].astype(jnp.float32))
    docx[1:9, :] = doc[...].astype(jnp.float32)

    def table_step(b, carry):
        rows = pl.ds(pl.multiple_of(b * WINDOW, WINDOW), WINDOW)
        cb = rope[2, pl.ds(place * NB + b, 1), :]
        sb = rope[3, pl.ds(place * NB + b, 1), :]
        cosv[rows, :] = rope[0] * cb - rope[1] * sb
        sinv[rows, :] = (rope[1] * cb + rope[0] * sb) * sign
        r = lax.broadcasted_iota(jnp.int32, (128, 128), 0)
        c = lax.broadcasted_iota(jnp.int32, (128, 128), 1)
        k0 = docx[pl.ds(b, 1), :]
        k1 = docx[pl.ds(b + 1, 1), :]
        mine = jnp.sum(jnp.where(r == c, k1, 0.0), axis=1, keepdims=True)
        bias[b, :, 0:128] = jnp.where(jnp.logical_and(c > r, k0 == mine), 0.0, NEG)
        bias[b, :, 128:256] = jnp.where(jnp.logical_and(c <= r, k1 == mine), 0.0, NEG)
        return carry

    lax.fori_loop(0, NB, table_step, 0)

    def spread(dst, g, rows, v):
        low = lax.broadcasted_iota(jnp.int32, v.shape, 1) < 64
        turned = pltpu.roll(v, 64, 1)
        dst[g, 0, rows, :] = jnp.where(low, v, 0.0).astype(jnp.bfloat16)
        dst[g, 1, rows, :] = jnp.where(low, 0.0, turned).astype(jnp.bfloat16)
        dst[g, 2, rows, :] = jnp.where(low, turned, 0.0).astype(jnp.bfloat16)
        dst[g, 3, rows, :] = jnp.where(low, 0.0, v).astype(jnp.bfloat16)

    def product(g, rows, a, b):
        weights = jnp.concatenate([w[g, a], w[g, b]], axis=1)
        return jnp.dot(mixed[rows, :], weights, preferred_element_type=jnp.float32)

    def turn(v, rows):
        low = lax.broadcasted_iota(jnp.int32, (ROWS, 128), 1) % 64 < 32
        swapped = jnp.where(low, pltpu.roll(v, 96, 1), pltpu.roll(v, 32, 1))
        return v * cosv[rows, :] + swapped * sinv[rows, :]

    def project_kv(g, start):
        rows = pl.ds(start, ROWS)
        ext = pl.ds(pl.multiple_of(start + WINDOW, WINDOW), ROWS)
        p = product(g, rows, 0, CHUNKS)
        k = turn(p[:, 0:128], rows)
        v = p[:, 128:256]
        spread(kx, g, ext, k)
        spread(vx, g, ext, v)
        tail[g, 0, :, :] = k[ROWS - WINDOW:].astype(jnp.bfloat16)
        tail[g, 1, :, :] = v[ROWS - WINDOW:].astype(jnp.bfloat16)

    def project_q(g, j, start):
        rows = pl.ds(start, ROWS)
        p = product(g, rows, 1 + j, CHUNKS + 1 + j)
        for i in range(2):
            v = turn(p[:, i * 128:(i + 1) * 128], rows) * 0.125
            q[g, j, i, rows, :] = v.astype(jnp.bfloat16)

    def kv_range(g):
        def step(i, carry):
            project_kv(g, pl.multiple_of(i * ROWS, ROWS))
            return carry

        lax.fori_loop(0, 2, step, 0)
        for i in range(2):
            kv_copy(g, i).start()

    def q_range(g, low, high):
        def step(i, carry):
            project_q(g, i // 2, pl.multiple_of((i % 2) * ROWS, ROWS))
            return carry

        lax.fori_loop(low, high, step, 0)

    def kv_copy(g, i):
        return remote(
            tail.at[g, i], halo.at[1 - g, i],
            kv_s.at[g, i], kv_r.at[1 - g, i], next_chip,
        )

    def attend(g, j, b):
        rows = pl.ds(pl.multiple_of(b * WINDOW, WINDOW), WINDOW)
        keys = pl.ds(pl.multiple_of(b * WINDOW, WINDOW), 2 * WINDOW)
        extra = bias[b]
        extra = jnp.concatenate([extra, extra], axis=0)
        low = lax.broadcasted_iota(jnp.int32, (256, 128), 1) < 64
        both = jnp.concatenate([q[g, j, 0, rows, :], q[g, j, 1, rows, :]], axis=0)
        k2 = jnp.concatenate([kx[g, 2 * j, keys, :], kx[g, 2 * j + 1, keys, :]], axis=0)
        v2 = jnp.concatenate([vx[g, 2 * j, keys, :], vx[g, 2 * j + 1, keys, :]], axis=0)
        s = lax.dot_general(both, k2, (((1,), (1,)), ((), ())), preferred_element_type=jnp.float32)
        weights, inverse = [], []
        for i in range(2):
            half = s[:, i * 256:(i + 1) * 256] + extra
            e = jnp.exp(half - jnp.max(half, axis=1, keepdims=True))
            inverse.append(1.0 / jnp.sum(e, axis=1, keepdims=True))
            weights.append(e.astype(jnp.bfloat16))
        o = jnp.dot(jnp.concatenate(weights, axis=1), v2, preferred_element_type=jnp.float32)
        o = (o * jnp.where(low, inverse[0], inverse[1])).astype(jnp.bfloat16)
        att[g, rows, j * 256:j * 256 + 128] = o[0:128]
        att[g, rows, j * 256 + 128:j * 256 + 256] = o[128:256]

    def attend_blocks(g, heads, low, high):
        def step(b, carry):
            for j in heads:
                attend(g, j, b)
            return carry

        lax.fori_loop(low, high, step, 0)

    def halo_in(g):
        for i in range(2):
            copy = remote(
                halo.at[g, i], halo.at[g, i], kv_s.at[1 - g, i], kv_r.at[g, i], prev_chip
            )
            copy.wait_recv()
        spread(kx, g, pl.ds(0, WINDOW), halo[g, 0].astype(jnp.float32))
        spread(vx, g, pl.ds(0, WINDOW), halo[g, 1].astype(jnp.float32))

    def out_product(g, blocks, features, start):
        weights = jnp.concatenate([w[g, b, features, :] for b, _ in blocks], axis=1)
        low, high = blocks[0][1] * 128, blocks[-1][1] * 128 + 128
        return lax.dot_general(
            weights, att[g, pl.ds(start, ROWS), low:high], (((1,), (1,)), ((), ())),
            preferred_element_type=jnp.float32,
        )

    def feature_rows(i):
        return pl.ds(pl.multiple_of(i * FC, 8), FC)

    both_parts = ((3, 0), (CHUNKS + 3, 1), (4, 2), (CHUNKS + 4, 3))

    def out_own(h):
        def step(i, carry):
            acc[h, feature_rows(i), :] = out_product(0, both_parts, feature_rows(i), h * ROWS)
            return carry

        lax.fori_loop(0, 4, step, 0)

    def out_add():
        def step(i, carry):
            for h in range(2):
                acc[h, feature_rows(i), :] += out_product(1, both_parts[:2], feature_rows(i), h * ROWS)
            return carry

        lax.fori_loop(0, 4, step, 0)

    def part_copy(i):
        rows = feature_rows(i)
        return remote(psend.at[rows], precv.at[rows], part_s.at[i], part_r.at[i], partner)

    def out_copy(i):
        rows = feature_rows(i)
        return pltpu.make_async_copy(flat.at[rows], out_h.at[rows], out_sem.at[i])

    def far_step(i, carry):
        rows = feature_rows(i)
        p = acc[1 - core, rows, :] + out_product(1, both_parts[2:], rows, other)
        psend[rows, :] = p.astype(jnp.bfloat16)
        part_copy(i).start()
        return carry

    def near_step(i, carry):
        rows = feature_rows(i)
        p = acc[core, rows, :] + out_product(1, both_parts[2:], rows, own)
        part_copy(i).wait_recv()
        p = p + precv[rows, :].astype(jnp.float32)
        flat[rows, :] = (flat[rows, :].astype(jnp.float32) + p).astype(jnp.bfloat16)
        out_copy(i).start()
        return carry

    for i in range(4, 10):
        loads[i].wait()
    for b in range(NCB):
        mix_copy(b, other).wait_recv()
    kv_range(0)
    slot(1)
    q_range(0, 0, 2)
    slot(2)
    q_range(0, 2, 4)
    slot(3)
    attend_blocks(0, (0, 1), 1, 3)
    slot(4)
    attend_blocks(0, (0, 1), 3, 6)
    slot(5)
    attend_blocks(0, (0, 1), 6, 8)
    slot(6)
    for i in range(10, 14):
        loads[i].wait()
    out_own(1)
    slot(7)
    s3(0)
    kv_range(1)
    slot(8)
    s3(1)
    q_range(1, 0, 2)
    slot(9)
    halo_in(1)
    attend_blocks(1, (0,), 0, NB)
    slot(10)
    halo_in(0)
    attend_blocks(0, (0, 1), 0, 1)
    out_own(0)
    slot(11)
    s3(2)
    q_range(1, 2, 4)
    slot(12)
    attend_blocks(1, (1,), 0, NB)
    slot(13)
    s3(3)
    out_add()
    slot(14)
    s3(4)
    lax.fori_loop(0, 4, far_step, 0)
    lax.fori_loop(0, 4, near_step, 0)

    for i in range(4):
        out_copy(i).wait()
        part_copy(i).wait_send()
    for b in range(NCB):
        mix_copy(b, own).wait_send()
    for g in range(2):
        for i in range(2):
            kv_copy(g, i).wait_send()
    for copy in sent:
        copy.wait_send()


def local(hidden_in, norm_gain, conv_weight, w_query, w_key, w_value, w_out, doc_ids):
    bf16, f32 = jnp.bfloat16, jnp.float32
    vmem, dma = pltpu.VMEM, pltpu.SemaphoreType.DMA
    scratch = [
        vmem((HALO + ROWS, D), bf16),
        vmem((D, ROWS), bf16),
        vmem((4, D), f32),
        vmem((CHIP, D), bf16),
        vmem((2, 2 * CHUNKS, D, 128), bf16),
        vmem((4, 128, 128), f32),
        vmem((CHIP, 128), f32),
        vmem((CHIP, 128), f32),
        vmem((8, 128), jnp.int32),
        vmem((8, 128), jnp.int32),
        vmem((16, 128), f32),
        vmem((NB, 128, 256), f32),
        vmem((2, 2, 2, CHIP, 128), bf16),
        vmem((2, 4, CHIP + WINDOW, 128), bf16),
        vmem((2, 4, CHIP + WINDOW, 128), bf16),
        vmem((2, 2, WINDOW, 128), bf16),
        vmem((2, 2, WINDOW, 128), bf16),
        vmem((2, CHIP, 512), bf16),
        vmem((2, D, ROWS), f32),
        vmem((D, ROWS), bf16),
        vmem((D, ROWS), bf16),
        dma((14,)),
        dma((2, CHUNKS, 8)),
        dma((2, CHUNKS, 8)),
        dma((NCB,)),
        dma((NCB,)),
        dma((2,)),
        dma((2,)),
        dma((2, 2)),
        dma((2, 2)),
        dma((4,)),
        dma((4,)),
        dma((4,)),
    ]
    hbm = pl.BlockSpec(memory_space=pl.ANY)
    out = pl.pallas_call(
        kernel,
        out_shape=jax.ShapeDtypeStruct((D, ROWS), bf16),
        in_specs=[hbm, pl.BlockSpec(memory_space=pltpu.VMEM), *[hbm] * 7],
        out_specs=hbm,
        scratch_shapes=scratch,
        compiler_params=pltpu.CompilerParams(
            collective_id=0, has_side_effects=True, vmem_limit_bytes=67043328
        ),
        name="attention_block",
    )(
        hidden_in.T, norm_gain, conv_weight, w_query, w_key, w_value, w_out.T,
        doc_ids.reshape(16, 128), jnp.asarray(rope_tables()),
    )
    return out.T


def solution(mesh):
    in_specs = (
        P(("dp", "seq", "tensor"), None),
        P(),
        P(),
        P(None, "tensor"),
        P(None, "tensor"),
        P(None, "tensor"),
        P("tensor", None),
        P(("dp", "seq")),
    )
    out_specs = P(("dp", "seq", "tensor"), None)
    return jax.shard_map(local, mesh=mesh, in_specs=in_specs, out_specs=out_specs, check_vma=False)
```

```python
import math

import jax
import jax.numpy as jnp
import numpy as np
from jax import lax
from jax.experimental import pallas as pl
from jax.experimental.pallas import tpu as pltpu
from jax.sharding import PartitionSpec as P

HEAD = 64
WINDOW = 128
EPS = 1e-05
ROPE_BASE = 150000.0
NEG = -1e30
MESH = pl.DeviceIdType.MESH

D = 2880
ROWS = 512
CHIP = 2 * ROWS
NB = CHIP // WINDOW
HALO = 16
TB = 256
FC = D // 4
CB = 64
NCB = ROWS // CB
PIECE = D // 8
CHUNKS = 5
BEFORE = {
    "kv1": ((5, 1, 0),),
    "q10": ((5, 0, 1), (5, 1, 1)),
    "q11": ((5, 1, 2),),
}
AFTER = {
    "norm": {7: ((0, 0, 0),)},
    "kv0": {1: ((0, 1, 0),), 2: ((0, 0, 1),)},
    "q0": {1: ((1, 0, 0), (2, 0, 0)), 2: ((0, 1, 1),), 3: ((1, 1, 0), (2, 1, 0)), 4: ((0, 0, 2), (2, 0, 1))},
    "own": {1: ((1, 0, 1),), 2: ((3, 0, 0), (4, 0, 0), (0, 1, 2)), 3: ((1, 1, 1), (2, 1, 1)), 4: ((0, 0, 3),), 5: ((3, 1, 0), (4, 1, 0)), 6: ((1, 0, 2),), 7: ((0, 1, 3), (2, 0, 2))},
    "of": {1: ((1, 1, 2), (3, 0, 1)), 2: ((0, 0, 4),), 3: ((5, 0, 0), (3, 1, 1), (2, 1, 2), (1, 0, 3)), 4: ((4, 0, 1), (0, 1, 4))},
    "kv1": {1: ((4, 1, 1), (1, 1, 3)), 2: ((2, 0, 3),)},
    "q10": {1: ((3, 0, 2), (3, 1, 2), (4, 0, 2), (4, 1, 2), (2, 1, 3), (1, 0, 4), (1, 1, 4)), 2: ((2, 0, 4),)},
    "ar0": {2: ((3, 0, 3),), 4: ((4, 0, 3),), 6: ((5, 0, 2), (3, 1, 3), (2, 1, 4))},
    "q11": {2: ((4, 1, 3), (3, 0, 4), (3, 1, 4), (4, 0, 4))},
    "ao0": {1: ((5, 0, 3),)},
    "ar1": {2: ((5, 1, 3), (4, 1, 4)), 8: ((5, 0, 4), (5, 1, 4))},
}
A, B, AL, AR, BL, BR, ALL_, BRR = range(8)


def rope_tables():
    half = HEAD // 2
    frequency = np.exp(np.arange(half) * (-2.0 * math.log(ROPE_BASE) / HEAD))
    lanes = np.tile(frequency, 4)
    inner = np.arange(WINDOW)[:, None] * lanes[None, :]
    outer = (np.arange(128) * WINDOW)[:, None] * lanes[None, :]
    return np.stack([np.cos(inner), np.sin(inner), np.cos(outer), np.sin(outer)]).astype(np.float32)


def kernel(
    hid_h, gain, conv_h, wq_h, wk_h, wv_h, wo_h, doc_h, rope_h, outv,
    hid, flat, conv, mixed, w, rope, cosv, sinv, doc, dprev, docx, bias,
    q, kx, vx, tail, halo, att, att2, w2, acc,
    load_sem, wsem_s, wsem_r, mix_s, mix_r, edge_s, edge_r, kv_s, kv_r, far_s, far_r, att_s, att_r,
):
    dp, seq, tensor = lax.axis_index("dp"), lax.axis_index("seq"), lax.axis_index("tensor")
    yh, core = tensor // 2, tensor % 2
    yl, x = seq // 4, seq % 4
    cross = (dp, (1 - yl) * 4 + x, (1 - yh) * 2 + core)
    ylo = (dp, (1 - yl) * 4 + x, tensor)
    right = ((dp, yl * 4 + (x + 1) % 4, tensor), ((dp + 1) % 4, seq, tensor))
    left = ((dp, yl * 4 + (x + 3) % 4, tensor), ((dp + 3) % 4, seq, tensor))
    partner = (dp, seq, yh * 2 + (1 - core))
    place = seq * 2 + yh
    nplace, pplace = (place + 1) % 16, (place + 15) % 16
    next_chip = (dp, nplace // 2, (nplace % 2) * 2 + core)
    prev_chip = (dp, pplace // 2, (pplace % 2) * 2 + core)
    order = seq * 4 + tensor
    norder, porder = (order + 1) % 32, (order + 31) % 32
    next_dev = (dp, norder // 4, norder % 4)
    prev_dev = (dp, porder // 4, porder % 4)
    ring = (x, dp)

    own = pl.multiple_of(core * ROWS, ROWS)
    other = pl.multiple_of((1 - core) * ROWS, ROWS)

    def local(i, src, dst):
        return pltpu.make_async_copy(src, dst, load_sem.at[i])

    doc_rows = pl.ds(pl.multiple_of(yh * 8, 8), 8)
    loads = [
        local(0, hid_h, flat),
        local(1, conv_h, conv),
        local(2, rope_h, rope),
        local(3, doc_h.at[doc_rows], doc),
        local(4, wk_h, w.at[0, 0]),
        local(5, wv_h, w.at[0, 5]),
    ]
    for j in range(4):
        cols = pl.ds(j * 128, 128)
        loads.append(local(6 + j, wq_h.at[:, cols], w.at[0, (j % 2) * 5 + 1 + j // 2]))
    for j in range(4):
        cols = pl.ds(j * 128, 128)
        loads.append(local(10 + j, wo_h.at[:, cols], w.at[0, (j % 2) * 5 + 3 + j // 2]))
    for load in loads:
        load.start()

    barrier = pltpu.get_barrier_semaphore()
    peers = [cross, ylo, *right, *left, partner, next_chip, prev_chip, next_dev, prev_dev]
    for peer in peers:
        pl.semaphore_signal(barrier, inc=1, device_id=peer, device_id_type=MESH)
    pl.semaphore_wait(barrier, len(peers))

    def remote(src, dst, send, recv, device):
        return pltpu.make_async_remote_copy(
            src_ref=src, dst_ref=dst, send_sem=send, recv_sem=recv,
            device_id=device, device_id_type=MESH,
        )

    def span(at, l):
        return pl.ds(pl.multiple_of(at * (2 * PIECE) + l * PIECE, 8), PIECE)

    def piece(s, c, at, l):
        return w.at[1, s * CHUNKS + c, span(at, l)]

    def source(s, c, at, l):
        if c == 0:
            return (wk_h, wv_h)[s].at[span(at, l)]
        ref = wq_h if c < 3 else wo_h
        return ref.at[span(at, l), pl.ds((((c - 1) % 2) * 2 + s) * 128, 128)]

    def before(s):
        return (ring[s] + 3) % 4

    def after(s):
        return (ring[s] + 1) % 4

    def over(s):
        return (ring[s] + 2) % 4

    def sends(s, c):
        mine, given = piece(s, c, ring[s], yl), piece(s, c, ring[s], 1 - yl)
        from_left, from_right = piece(s, c, before(s), yl), piece(s, c, after(s), 1 - yl)
        return {
            A: (source(s, c, ring[s], 1 - yl), given, cross),
            B: (mine, mine, ylo),
            AL: (mine, mine, right[s]),
            AR: (mine, mine, left[s]),
            BL: (given, given, right[s]),
            BR: (given, given, left[s]),
            ALL_: (from_left, from_left, right[s]),
            BRR: (from_right, from_right, left[s]),
        }

    def sending(s, c, kind):
        src, dst, device = sends(s, c)[kind]
        return remote(src, dst, wsem_s.at[s, c, kind], wsem_r.at[s, c, kind], device)

    def arrived(s, c, kind):
        at, l = {
            A: (ring[s], yl), B: (ring[s], 1 - yl), AL: (before(s), yl), AR: (after(s), yl),
            BL: (before(s), 1 - yl), BR: (after(s), 1 - yl), ALL_: (over(s), yl), BRR: (over(s), 1 - yl),
        }[kind]
        ref = piece(s, c, at, l)
        remote(ref, ref, wsem_s.at[s, c, kind], wsem_r.at[s, c, kind], cross).wait_recv()

    def far_copy(s, c, k):
        at = (ring[s], before(s), after(s), over(s))[k]
        rows = pl.ds(pl.multiple_of(at * (2 * PIECE), 16), 2 * PIECE)
        sems = far_s.at[s, c - 2, k], far_r.at[s, c - 2, k]
        return remote(w.at[1, s * CHUNKS + c, rows], w2.at[1, (c - 3) * 2 + s, rows], *sems, partner)

    stages = (
        ((A,), (AL, AR, B), ()),
        ((B,), (BR, BL), (0,)),
        ((AL,), (ALL_,), ()),
        ((BR,), (BRR,), ()),
        ((AR, BL), (), (1, 2)),
        ((ALL_, BRR), (), (3,)),
    )

    def run(steps):
        for stage, s, c in steps:
            awaited, forwarded, complete = stages[stage]
            for kind in awaited:
                arrived(s, c, kind)
            for kind in forwarded:
                sending(s, c, kind).start()
            if c >= 3:
                for k in complete:
                    far_copy(s, c, k).start()

    zero = core // 2

    def phase(name, low, high, body, hooks=()):
        run(BEFORE.get(name, ()))

        def step(i, carry):
            body(i)
            return carry

        at, hooks, steps = low, dict(hooks), AFTER.get(name, {})
        for count in sorted({*hooks, *steps}):
            lax.fori_loop(at + zero, low + count, step, 0)
            hooks.get(count, lambda: None)()
            run(steps.get(count, ()))
            at = low + count
        if at < high:
            lax.fori_loop(at, high, step, 0)

    def wo_copy(j):
        src = wo_h.at[:, pl.ds(j * 128, 128)]
        return remote(src, w2.at[0, j], far_s.at[j // 2, 0, j % 2], far_r.at[j // 2, 0, j % 2], partner)

    def before(s):
        return (ring[s] + 3) % 4

    def after(s):
        return (ring[s] + 1) % 4

    def over(s):
        return (ring[s] + 2) % 4

    def s0(c):
        for s in range(2):
            arrived(s, c, A, ring[s], yl)
            ref = piece(s, c, ring[s], yl)
            send(s, c, AL, ref, ref, right[s])
            send(s, c, AR, ref, ref, left[s])
            send(s, c, B, ref, ref, ylo)

    def s1(c):
        for s in range(2):
            arrived(s, c, B, ring[s], 1 - yl)
            ref = piece(s, c, ring[s], 1 - yl)
            send(s, c, BR, ref, ref, left[s])
            send(s, c, BL, ref, ref, right[s])
            arrived(s, c, AL, before(s), yl)
            ref = piece(s, c, before(s), yl)
            send(s, c, ALL_, ref, ref, right[s])

    def s2(c):
        for s in range(2):
            arrived(s, c, BR, after(s), 1 - yl)
            ref = piece(s, c, after(s), 1 - yl)
            send(s, c, BRR, ref, ref, left[s])

    def s3(c):
        for s in range(2):
            arrived(s, c, AR, after(s), yl)
            arrived(s, c, BL, before(s), 1 - yl)
            arrived(s, c, ALL_, over(s), yl)
            arrived(s, c, BRR, over(s), 1 - yl)

    def far_arrived(c):
        for s in range(2):
            for k in range(4):
                far_copy(s, c, k).wait_recv()

    edge = [
        remote(hid.at[pl.ds(HALO + ROWS - 8, 8)], hid.at[pl.ds(8, 8)], edge_s.at[0], edge_r.at[0], next_dev),
        remote(doc_h.at[doc_rows], dprev, edge_s.at[1], edge_r.at[1], next_chip),
    ]
    for c in range(CHUNKS):
        for s in range(2):
            sending(s, c, A).start()
    edge[1].start()

    for i in range(2):
        loads[i].wait()
    unit = lax.broadcasted_iota(jnp.int32, (TB, TB), 0) == lax.broadcasted_iota(jnp.int32, (TB, TB), 1)
    unit = jnp.where(unit, 1.0, 0.0).astype(jnp.bfloat16)

    def transpose(i):
        for f in range(0, D, 768):
            rows = slice(f, min(f + 768, D))
            turned = lax.dot_general(
                unit, flat[rows, i * TB:(i + 1) * TB], (((1,), (1,)), ((), ())),
                preferred_element_type=jnp.float32,
            )
            hid[HALO + i * TB:HALO + (i + 1) * TB, rows] = turned.astype(jnp.bfloat16)

    transpose(1)
    transpose(0)
    edge[0].start()

    def norm_conv(b):
        base = pl.multiple_of(b * CB, CB)
        rows = pl.ds(base, CB + HALO)
        total = jnp.zeros((CB + 8, 128), jnp.float32)
        for lane in range(0, D - 64, 128):
            v = hid[rows, lane:lane + 128].astype(jnp.float32)[8:]
            total = total + v * v
        v = hid[rows, D - 64:D].astype(jnp.float32)[8:]
        square = jnp.sum(total, axis=1, keepdims=True) + jnp.sum(v * v, axis=1, keepdims=True)
        scale = lax.rsqrt(square * (1.0 / D) + EPS)
        first = jnp.logical_and(b == 0, order == 0)
        row = lax.broadcasted_iota(jnp.int32, (CB + 8, 1), 0)
        keep = jnp.where(first, 0.0, 1.0)
        scale = jnp.where(row < 8, scale * keep, scale)
        at = pl.multiple_of(own + base, CB)
        for lane in range(0, D, 128):
            width = min(128, D - lane)
            cols = slice(lane, lane + width)
            v = hid[rows, cols].astype(jnp.float32)[8:]
            n = (v * scale * gain[cols].reshape(1, width)).astype(jnp.bfloat16).astype(jnp.float32)
            m = conv[0:1, cols] * n[8:]
            for tap in range(1, 4):
                m = m + conv[tap:tap + 1, cols] * pltpu.roll(n, tap, 0)[8:]
            mixed[pl.ds(at, CB), cols] = m.astype(jnp.bfloat16)

    def mix_copy(b, start):
        rows = pl.ds(pl.multiple_of(start + b * CB, CB), CB)
        return remote(mixed.at[rows], mixed.at[rows], mix_s.at[b], mix_r.at[b], partner)

    def norm_step(i):
        b = (i + 1) % NCB

        @pl.when(i == NCB - 1)
        def _():
            edge[0].wait()

        norm_conv(b)
        mix_copy(b, own).start()

    phase("norm", 0, NCB, norm_step)

    loads[2].wait()
    loads[3].wait()
    edge[1].wait()
    lane = lax.broadcasted_iota(jnp.int32, (1, 128), 1)
    sign = jnp.where(lane % 64 < 32, -1.0, 1.0)
    docx[0:1, :] = jnp.where(place == 0, -1.0, dprev[7:8, :].astype(jnp.float32))
    docx[1:9, :] = doc[...].astype(jnp.float32)

    def table_step(b):
        rows = pl.ds(pl.multiple_of(b * WINDOW, WINDOW), WINDOW)
        cb = rope[2, pl.ds(place * NB + b, 1), :]
        sb = rope[3, pl.ds(place * NB + b, 1), :]
        cosv[rows, :] = rope[0] * cb - rope[1] * sb
        sinv[rows, :] = (rope[1] * cb + rope[0] * sb) * sign
        r = lax.broadcasted_iota(jnp.int32, (128, 128), 0)
        c = lax.broadcasted_iota(jnp.int32, (128, 128), 1)
        k0 = docx[pl.ds(b, 1), :]
        k1 = docx[pl.ds(b + 1, 1), :]
        mine = jnp.sum(jnp.where(r == c, k1, 0.0), axis=1, keepdims=True)
        bias[b, :, 0:128] = jnp.where(jnp.logical_and(c > r, k0 == mine), 0.0, NEG)
        bias[b, :, 128:256] = jnp.where(jnp.logical_and(c <= r, k1 == mine), 0.0, NEG)

    lax.fori_loop(0, NB, lambda b, carry: table_step(b), None)
    run(AFTER.get("table", {}).get(1, ()))

    def spread(dst, g, rows, v):
        low = lax.broadcasted_iota(jnp.int32, v.shape, 1) < 64
        turned = pltpu.roll(v, 64, 1)
        dst[g, 0, rows, :] = jnp.where(low, v, 0.0).astype(jnp.bfloat16)
        dst[g, 1, rows, :] = jnp.where(low, 0.0, turned).astype(jnp.bfloat16)
        dst[g, 2, rows, :] = jnp.where(low, turned, 0.0).astype(jnp.bfloat16)
        dst[g, 3, rows, :] = jnp.where(low, 0.0, v).astype(jnp.bfloat16)

    def product(g, rows, a, b):
        weights = jnp.concatenate([w[g, a], w[g, b]], axis=1)
        return jnp.dot(mixed[rows, :], weights, preferred_element_type=jnp.float32)

    def turn(v, rows):
        low = lax.broadcasted_iota(jnp.int32, (ROWS, 128), 1) % 64 < 32
        swapped = jnp.where(low, pltpu.roll(v, 96, 1), pltpu.roll(v, 32, 1))
        return v * cosv[rows, :] + swapped * sinv[rows, :]

    def project_kv(g, start):
        rows = pl.ds(start, ROWS)
        ext = pl.ds(pl.multiple_of(start + WINDOW, WINDOW), ROWS)
        p = product(g, rows, 0, CHUNKS)
        k = turn(p[:, 0:128], rows)
        v = p[:, 128:256]
        spread(kx, g, ext, k)
        spread(vx, g, ext, v)
        tail[g, 0, :, :] = k[ROWS - WINDOW:].astype(jnp.bfloat16)
        tail[g, 1, :, :] = v[ROWS - WINDOW:].astype(jnp.bfloat16)

    def project_q(g, j, start):
        rows = pl.ds(start, ROWS)
        p = product(g, rows, 1 + j, CHUNKS + 1 + j)
        for i in range(2):
            v = turn(p[:, i * 128:(i + 1) * 128], rows) * 0.125
            q[g, j, i, rows, :] = v.astype(jnp.bfloat16)

    def kv_phase(name, g):
        phase(name, 0, 2, lambda i: project_kv(g, pl.multiple_of(i * ROWS, ROWS)))
        for i in range(2):
            kv_copy(g, i).start()

    def q_phase(name, g, low, high):
        phase(
            name, low, high,
            lambda i: project_q(g, i // 2, pl.multiple_of((i % 2) * ROWS, ROWS)),
        )

    def kv_copy(g, i):
        return remote(
            tail.at[g, i], halo.at[1 - g, i],
            kv_s.at[g, i], kv_r.at[1 - g, i], next_chip,
        )

    def attend(g, j, b):
        rows = pl.ds(pl.multiple_of(b * WINDOW, WINDOW), WINDOW)
        keys = pl.ds(pl.multiple_of(b * WINDOW, WINDOW), 2 * WINDOW)
        extra = bias[b]
        extra = jnp.concatenate([extra, extra], axis=0)
        low = lax.broadcasted_iota(jnp.int32, (256, 128), 1) < 64
        both = jnp.concatenate([q[g, j, 0, rows, :], q[g, j, 1, rows, :]], axis=0)
        k2 = jnp.concatenate([kx[g, 2 * j, keys, :], kx[g, 2 * j + 1, keys, :]], axis=0)
        v2 = jnp.concatenate([vx[g, 2 * j, keys, :], vx[g, 2 * j + 1, keys, :]], axis=0)
        s = lax.dot_general(both, k2, (((1,), (1,)), ((), ())), preferred_element_type=jnp.float32)
        weights, inverse = [], []
        for i in range(2):
            half = s[:, i * 256:(i + 1) * 256] + extra
            e = jnp.exp(half - jnp.max(half, axis=1, keepdims=True))
            inverse.append(1.0 / jnp.sum(e, axis=1, keepdims=True))
            weights.append(e.astype(jnp.bfloat16))
        o = jnp.dot(jnp.concatenate(weights, axis=1), v2, preferred_element_type=jnp.float32)
        o = (o * jnp.where(low, inverse[0], inverse[1])).astype(jnp.bfloat16)
        att[g, j, rows, 0:128] = o[0:128]
        att[g, j, rows, 128:256] = o[128:256]

    def attend_phase(name, g, heads, low, high, sent):
        count = high - low

        def body(i):
            b = low + (i + (count // 2) * (1 - core)) % count
            for j in heads:
                attend(g, j, b)

        def leave():
            for j in heads:
                att_copy(sent, j).start()

        phase(name, 0, count, body, {min(4, count): leave})

    def halo_in(g):
        for i in range(2):
            copy = remote(
                halo.at[g, i], halo.at[g, i], kv_s.at[1 - g, i], kv_r.at[g, i], prev_chip
            )
            copy.wait_recv()
        spread(kx, g, pl.ds(0, WINDOW), halo[g, 0].astype(jnp.float32))
        spread(vx, g, pl.ds(0, WINDOW), halo[g, 1].astype(jnp.float32))

    def att_copy(k, j):
        g = k // 2
        start, count = ((128, ROWS - 128), (0, 128), (0, ROWS))[k]
        rows = pl.ds(pl.multiple_of(other + start, 128), count)
        dst = att2.at[g, j, pl.ds(start, count)]
        return remote(att.at[g, j, rows], dst, att_s.at[k, j], att_r.at[k, j], partner)

    def out_product(units, features, start, count):
        weights, heads = [], []
        rows = pl.ds(pl.multiple_of(own + start, 128), count)
        for g, j in units:
            weights += [w[g, 3 + j, features, :], w[g, CHUNKS + 3 + j, features, :]]
            weights += [w2[g, 2 * j, features, :], w2[g, 2 * j + 1, features, :]]
            heads += [att[g, j, rows, :], att2[g, j, start:start + count, :]]
        return lax.dot_general(
            jnp.concatenate(weights, axis=1), jnp.concatenate(heads, axis=1),
            (((1,), (1,)), ((), ())), preferred_element_type=jnp.float32,
        )

    def feature_rows(i):
        return pl.ds(pl.multiple_of(i * FC, 8), FC)

    near = ((0, 0), (0, 1))

    def out_near(i):
        rows = feature_rows(i)
        acc[rows, 128:ROWS] = out_product(near, rows, 128, ROWS - 128)

    def out_first(i):
        rows = feature_rows(i)
        acc[rows, 0:128] = out_product(near, rows, 0, 128)

    def out_next(i):
        rows = feature_rows(i)
        acc[rows, :] += out_product(((1, 0),), rows, 0, ROWS)

    def out_last(i):
        rows = feature_rows(i)
        p = acc[rows, :] + out_product(((1, 1),), rows, 0, ROWS)
        outv[rows, :] = (flat[rows, :].astype(jnp.float32) + p).astype(jnp.bfloat16)

    for i in range(4, 10):
        loads[i].wait()
    for b in range(NCB):
        mix_copy(b, other).wait_recv()
    for j in range(4):
        wo_copy(j).start()
    kv_phase("kv0", 0)
    q_phase("q0", 0, 0, 4)
    attend_phase("own", 0, (0, 1), 1, NB, 0)
    for i in range(10, 14):
        loads[i].wait()
    for j in range(4):
        wo_copy(j).wait_recv()
    for j in range(2):
        att_copy(0, j).wait_recv()
    phase("of", 0, 4, out_near)
    kv_phase("kv1", 1)
    q_phase("q10", 1, 0, 2)
    halo_in(1)
    attend_phase("ar0", 1, (0,), 0, NB, 2)
    q_phase("q11", 1, 2, 4)
    halo_in(0)
    attend_phase("ao0", 0, (0, 1), 0, 1, 1)
    attend_phase("ar1", 1, (1,), 0, NB, 2)
    for j in range(2):
        att_copy(1, j).wait_recv()
    phase("of2", 0, 4, out_first)
    run(BEFORE.get("on", ()))
    far_arrived(3)
    att_copy(2, 0).wait_recv()
    lax.fori_loop(0, 4, lambda i, carry: out_next(i), None)
    run(BEFORE.get("ol", ()))
    far_arrived(4)
    att_copy(2, 1).wait_recv()
    lax.fori_loop(0, 4, lambda i, carry: out_last(i), None)

    for b in range(NCB):
        mix_copy(b, own).wait_send()
    for j in range(4):
        wo_copy(j).wait_send()
    for i in range(2):
        for g in range(2):
            kv_copy(g, i).wait_send()
        for k in range(3):
            att_copy(k, i).wait_send()
    for s in range(2):
        for c in range(CHUNKS):
            for kind in range(8):
                sending(s, c, kind).wait_send()
            if c >= 3:
                for k in range(4):
                    far_copy(s, c, k).wait_send()


def local(hidden_in, norm_gain, conv_weight, w_query, w_key, w_value, w_out, doc_ids):
    bf16, f32 = jnp.bfloat16, jnp.float32
    vmem, dma = pltpu.VMEM, pltpu.SemaphoreType.DMA
    scratch = [
        vmem((HALO + ROWS, D), bf16),
        vmem((D, ROWS), bf16),
        vmem((4, D), f32),
        vmem((CHIP, D), bf16),
        vmem((2, 2 * CHUNKS, D, 128), bf16),
        vmem((4, 128, 128), f32),
        vmem((CHIP, 128), f32),
        vmem((CHIP, 128), f32),
        vmem((8, 128), jnp.int32),
        vmem((8, 128), jnp.int32),
        vmem((16, 128), f32),
        vmem((NB, 128, 256), f32),
        vmem((2, 2, 2, CHIP, 128), bf16),
        vmem((2, 4, CHIP + WINDOW, 128), bf16),
        vmem((2, 4, CHIP + WINDOW, 128), bf16),
        vmem((2, 2, WINDOW, 128), bf16),
        vmem((2, 2, WINDOW, 128), bf16),
        vmem((2, 2, CHIP, 256), bf16),
        vmem((2, 2, ROWS, 256), bf16),
        vmem((2, 4, D, 128), bf16),
        vmem((D, ROWS), f32),
        dma((14,)),
        dma((2, CHUNKS, 8)),
        dma((2, CHUNKS, 8)),
        dma((NCB,)),
        dma((NCB,)),
        dma((2,)),
        dma((2,)),
        dma((2, 2)),
        dma((2, 2)),
        dma((2, 3, 4)),
        dma((2, 3, 4)),
        dma((3, 2)),
        dma((3, 2)),
    ]
    hbm = pl.BlockSpec(memory_space=pl.ANY)
    out = pl.pallas_call(
        kernel,
        out_shape=pltpu.VMEM((D, ROWS), bf16),
        in_specs=[hbm, pl.BlockSpec(memory_space=pltpu.VMEM), *[hbm] * 7],
        out_specs=pl.BlockSpec(memory_space=pltpu.VMEM),
        scratch_shapes=scratch,
        compiler_params=pltpu.CompilerParams(
            collective_id=0, has_side_effects=True, vmem_limit_bytes=60 << 20
        ),
        name="attention_block",
    )(
        hidden_in.T, norm_gain, conv_weight, w_query, w_key, w_value, w_out.T,
        doc_ids.reshape(16, 128), jnp.asarray(rope_tables()),
    )
    return out.T


def solution(mesh):
    in_specs = (
        P(("dp", "seq", "tensor"), None),
        P(),
        P(),
        P(None, "tensor"),
        P(None, "tensor"),
        P(None, "tensor"),
        P("tensor", None),
        P(("dp", "seq")),
    )
    out_specs = P(("dp", "seq", "tensor"), None)
    return jax.shard_map(local, mesh=mesh, in_specs=in_specs, out_specs=out_specs, check_vma=False)
```

```python
import math

import jax
import jax.numpy as jnp
import numpy as np
from jax import lax
from jax.experimental import pallas as pl
from jax.experimental.pallas import tpu as pltpu
from jax.sharding import PartitionSpec as P

HEAD = 64
WINDOW = 128
EPS = 1e-05
ROPE_BASE = 150000.0
NEG = -1e30
MESH = pl.DeviceIdType.MESH

D = 2880
ROWS = 512
CHIP = 2 * ROWS
NB = CHIP // WINDOW
HALO = 16
TB = 256
FC = D // 4
CB = 64
NCB = ROWS // CB
UNITS = 2
PIECE = D // 8
CHUNKS = 5
BEFORE = {
    "kv1": ((5, 1, 0),),
    "q10": ((5, 0, 1), (5, 1, 1)),
    "q11": ((5, 1, 2),),
}
AFTER = {
    "norm": {7: ((0, 0, 0),)},
    "kv0": {1: ((0, 1, 0),), 2: ((0, 0, 1),)},
    "q0": {1: ((1, 0, 0), (2, 0, 0)), 2: ((0, 1, 1),), 3: ((1, 1, 0), (2, 1, 0), (0, 0, 2)), 4: ((1, 0, 1), (2, 0, 1))},
    "own": {1: ((0, 1, 2),), 2: ((3, 0, 0), (4, 0, 0)), 3: ((1, 1, 1), (2, 1, 1)), 4: ((0, 0, 3),), 6: ((3, 1, 0), (4, 1, 0), (1, 0, 2)), 7: ((0, 1, 3),)},
    "of": {1: ((1, 1, 2), (3, 0, 1), (2, 0, 2)), 2: ((0, 0, 4),), 3: ((5, 0, 0), (3, 1, 1), (4, 0, 1), (2, 1, 2), (1, 0, 3)), 4: ((0, 1, 4),)},
    "kv1": {1: ((4, 1, 1), (1, 1, 3)), 2: ((3, 0, 2), (2, 0, 3))},
    "q10": {1: ((3, 1, 2), (4, 0, 2), (4, 1, 2), (2, 1, 3), (1, 0, 4), (1, 1, 4)), 2: ((3, 0, 3), (2, 0, 4))},
    "ar0": {2: ((5, 0, 2), (4, 0, 3)), 4: ((3, 1, 3), (2, 1, 4))},
    "q11": {2: ((4, 1, 3), (5, 0, 3), (3, 0, 4), (3, 1, 4), (4, 0, 4))},
    "ar1": {2: ((5, 1, 3), (4, 1, 4)), 4: ((5, 0, 4), (5, 1, 4))},
}
A, B, AL, AR, BL, BR, ALL_, BRR = range(8)


def rope_tables():
    half = HEAD // 2
    frequency = np.exp(np.arange(half) * (-2.0 * math.log(ROPE_BASE) / HEAD))
    lanes = np.tile(frequency, 4)
    inner = np.arange(WINDOW)[:, None] * lanes[None, :]
    outer = (np.arange(128) * WINDOW)[:, None] * lanes[None, :]
    return np.stack([np.cos(inner), np.sin(inner), np.cos(outer), np.sin(outer)]).astype(np.float32)


def kernel(
    hid_h, gain, conv_h, wq_h, wk_h, wv_h, wo_h, doc_h, rope_h, outv,
    hid, flat, conv, mixed, w, rope, cosv, sinv, doc, dprev, docx, bias,
    q, kx, vx, tail, halo, att, att2, w2, acc,
    load_sem, wsem_s, wsem_r, mix_s, mix_r, edge_s, edge_r, kv_s, kv_r, far_s, far_r, att_s, att_r,
):
    dp, seq, tensor = lax.axis_index("dp"), lax.axis_index("seq"), lax.axis_index("tensor")
    yh, core = tensor // 2, tensor % 2
    yl, x = seq // 4, seq % 4
    cross = (dp, (1 - yl) * 4 + x, (1 - yh) * 2 + core)
    ylo = (dp, (1 - yl) * 4 + x, tensor)
    right = ((dp, yl * 4 + (x + 1) % 4, tensor), ((dp + 1) % 4, seq, tensor))
    left = ((dp, yl * 4 + (x + 3) % 4, tensor), ((dp + 3) % 4, seq, tensor))
    partner = (dp, seq, yh * 2 + (1 - core))
    place = seq * 2 + yh
    nplace, pplace = (place + 1) % 16, (place + 15) % 16
    next_chip = (dp, nplace // 2, (nplace % 2) * 2 + core)
    prev_chip = (dp, pplace // 2, (pplace % 2) * 2 + core)
    order = seq * 4 + tensor
    norder, porder = (order + 1) % 32, (order + 31) % 32
    next_dev = (dp, norder // 4, norder % 4)
    prev_dev = (dp, porder // 4, porder % 4)
    ring = (x, dp)

    own = pl.multiple_of(core * ROWS, ROWS)
    other = pl.multiple_of((1 - core) * ROWS, ROWS)

    def local(i, src, dst):
        return pltpu.make_async_copy(src, dst, load_sem.at[i])

    doc_rows = pl.ds(pl.multiple_of(yh * 8, 8), 8)
    loads = [
        local(0, hid_h, flat),
        local(1, conv_h, conv),
        local(2, rope_h, rope),
        local(3, doc_h.at[doc_rows], doc),
        local(4, wk_h, w.at[0, 0]),
        local(5, wv_h, w.at[0, 5]),
    ]
    for j in range(4):
        cols = pl.ds(j * 128, 128)
        loads.append(local(6 + j, wq_h.at[:, cols], w.at[0, (j % 2) * 5 + 1 + j // 2]))
    for j in range(4):
        cols = pl.ds(j * 128, 128)
        loads.append(local(10 + j, wo_h.at[:, cols], w.at[0, (j % 2) * 5 + 3 + j // 2]))
    for load in loads:
        load.start()

    barrier = pltpu.get_barrier_semaphore()
    peers = [cross, ylo, *right, *left, partner, next_chip, prev_chip, next_dev, prev_dev]
    for peer in peers:
        pl.semaphore_signal(barrier, inc=1, device_id=peer, device_id_type=MESH)
    pl.semaphore_wait(barrier, len(peers))

    def remote(src, dst, send, recv, device):
        return pltpu.make_async_remote_copy(
            src_ref=src, dst_ref=dst, send_sem=send, recv_sem=recv,
            device_id=device, device_id_type=MESH,
        )

    def span(at, l):
        return pl.ds(pl.multiple_of(at * (2 * PIECE) + l * PIECE, 8), PIECE)

    def piece(s, c, at, l):
        return w.at[1, s * CHUNKS + c, span(at, l)]

    def source(s, c, at, l):
        if c == 0:
            return (wk_h, wv_h)[s].at[span(at, l)]
        ref = wq_h if c < 3 else wo_h
        return ref.at[span(at, l), pl.ds((((c - 1) % 2) * 2 + s) * 128, 128)]

    def before(s):
        return (ring[s] + 3) % 4

    def after(s):
        return (ring[s] + 1) % 4

    def over(s):
        return (ring[s] + 2) % 4

    def sends(s, c):
        mine, given = piece(s, c, ring[s], yl), piece(s, c, ring[s], 1 - yl)
        from_left, from_right = piece(s, c, before(s), yl), piece(s, c, after(s), 1 - yl)
        return {
            A: (source(s, c, ring[s], 1 - yl), given, cross),
            B: (mine, mine, ylo),
            AL: (mine, mine, right[s]),
            AR: (mine, mine, left[s]),
            BL: (given, given, right[s]),
            BR: (given, given, left[s]),
            ALL_: (from_left, from_left, right[s]),
            BRR: (from_right, from_right, left[s]),
        }

    def sending(s, c, kind):
        src, dst, device = sends(s, c)[kind]
        return remote(src, dst, wsem_s.at[s, c, kind], wsem_r.at[s, c, kind], device)

    def arrived(s, c, kind):
        at, l = {
            A: (ring[s], yl), B: (ring[s], 1 - yl), AL: (before(s), yl), AR: (after(s), yl),
            BL: (before(s), 1 - yl), BR: (after(s), 1 - yl), ALL_: (over(s), yl), BRR: (over(s), 1 - yl),
        }[kind]
        ref = piece(s, c, at, l)
        remote(ref, ref, wsem_s.at[s, c, kind], wsem_r.at[s, c, kind], cross).wait_recv()

    def far_copy(s, c, k):
        at = (ring[s], before(s), after(s), over(s))[k]
        rows = pl.ds(pl.multiple_of(at * (2 * PIECE), 16), 2 * PIECE)
        sems = far_s.at[s, c - 2, k], far_r.at[s, c - 2, k]
        return remote(w.at[1, s * CHUNKS + c, rows], w2.at[1, (c - 3) * 2 + s, rows], *sems, partner)

    stages = (
        ((A,), (AL, AR, B), ()),
        ((B,), (BR, BL), (0,)),
        ((AL,), (ALL_,), ()),
        ((BR,), (BRR,), ()),
        ((AR, BL), (), (1, 2)),
        ((ALL_, BRR), (), (3,)),
    )

    def run(steps):
        for stage, s, c in steps:
            awaited, forwarded, complete = stages[stage]
            for kind in awaited:
                arrived(s, c, kind)
            for kind in forwarded:
                sending(s, c, kind).start()
            if c >= 3:
                for k in complete:
                    far_copy(s, c, k).start()

    zero = core // 2

    def phase(name, low, high, body, hooks=()):
        run(BEFORE.get(name, ()))

        def step(i, carry):
            body(i)
            return carry

        at, hooks, steps = low, dict(hooks), AFTER.get(name, {})
        for count in sorted({*hooks, *steps}):
            lax.fori_loop(at + zero, low + count, step, 0)
            hooks.get(count, lambda: None)()
            run(steps.get(count, ()))
            at = low + count
        if at < high:
            lax.fori_loop(at, high, step, 0)

    def wo_copy(j):
        src = wo_h.at[:, pl.ds(j * 128, 128)]
        return remote(src, w2.at[0, j], far_s.at[j // 2, 0, j % 2], far_r.at[j // 2, 0, j % 2], partner)

    def before(s):
        return (ring[s] + 3) % 4

    def after(s):
        return (ring[s] + 1) % 4

    def over(s):
        return (ring[s] + 2) % 4

    def s0(c):
        for s in range(2):
            arrived(s, c, A, ring[s], yl)
            ref = piece(s, c, ring[s], yl)
            send(s, c, AL, ref, ref, right[s])
            send(s, c, AR, ref, ref, left[s])
            send(s, c, B, ref, ref, ylo)

    def s1(c):
        for s in range(2):
            arrived(s, c, B, ring[s], 1 - yl)
            ref = piece(s, c, ring[s], 1 - yl)
            send(s, c, BR, ref, ref, left[s])
            send(s, c, BL, ref, ref, right[s])
            arrived(s, c, AL, before(s), yl)
            ref = piece(s, c, before(s), yl)
            send(s, c, ALL_, ref, ref, right[s])

    def s2(c):
        for s in range(2):
            arrived(s, c, BR, after(s), 1 - yl)
            ref = piece(s, c, after(s), 1 - yl)
            send(s, c, BRR, ref, ref, left[s])

    def s3(c):
        for s in range(2):
            arrived(s, c, AR, after(s), yl)
            arrived(s, c, BL, before(s), 1 - yl)
            arrived(s, c, ALL_, over(s), yl)
            arrived(s, c, BRR, over(s), 1 - yl)

    def far_arrived(c):
        for s in range(2):
            for k in range(4):
                far_copy(s, c, k).wait_recv()

    edge = [
        remote(hid.at[pl.ds(HALO + ROWS - 8, 8)], hid.at[pl.ds(8, 8)], edge_s.at[0], edge_r.at[0], next_dev),
        remote(doc_h.at[doc_rows], dprev, edge_s.at[1], edge_r.at[1], next_chip),
    ]
    for c in range(CHUNKS):
        for s in range(2):
            sending(s, c, A).start()
    edge[1].start()

    for i in range(2):
        loads[i].wait()
    unit = lax.broadcasted_iota(jnp.int32, (TB, TB), 0) == lax.broadcasted_iota(jnp.int32, (TB, TB), 1)
    unit = jnp.where(unit, 1.0, 0.0).astype(jnp.bfloat16)

    def transpose(i):
        for f in range(0, D, 768):
            rows = slice(f, min(f + 768, D))
            turned = lax.dot_general(
                unit, flat[rows, i * TB:(i + 1) * TB], (((1,), (1,)), ((), ())),
                preferred_element_type=jnp.float32,
            )
            hid[HALO + i * TB:HALO + (i + 1) * TB, rows] = turned.astype(jnp.bfloat16)

    transpose(1)
    transpose(0)
    edge[0].start()

    def norm_conv(b):
        base = pl.multiple_of(b * CB, CB)
        rows = pl.ds(base, CB + HALO)
        total = jnp.zeros((CB + 8, 128), jnp.float32)
        for lane in range(0, D - 64, 128):
            v = hid[rows, lane:lane + 128].astype(jnp.float32)[8:]
            total = total + v * v
        v = hid[rows, D - 64:D].astype(jnp.float32)[8:]
        square = jnp.sum(total, axis=1, keepdims=True) + jnp.sum(v * v, axis=1, keepdims=True)
        scale = lax.rsqrt(square * (1.0 / D) + EPS)
        first = jnp.logical_and(b == 0, order == 0)
        row = lax.broadcasted_iota(jnp.int32, (CB + 8, 1), 0)
        keep = jnp.where(first, 0.0, 1.0)
        scale = jnp.where(row < 8, scale * keep, scale)
        at = pl.multiple_of(own + base, CB)
        for lane in range(0, D, 128):
            width = min(128, D - lane)
            cols = slice(lane, lane + width)
            v = hid[rows, cols].astype(jnp.float32)[8:]
            n = (v * scale * gain[cols].reshape(1, width)).astype(jnp.bfloat16).astype(jnp.float32)
            m = conv[0:1, cols] * n[8:]
            for tap in range(1, 4):
                m = m + conv[tap:tap + 1, cols] * pltpu.roll(n, tap, 0)[8:]
            mixed[pl.ds(at, CB), cols] = m.astype(jnp.bfloat16)

    def mix_copy(b, start):
        rows = pl.ds(pl.multiple_of(start + b * CB, CB), CB)
        return remote(mixed.at[rows], mixed.at[rows], mix_s.at[b], mix_r.at[b], partner)

    def norm_step(i):
        b = (i + 1) % NCB

        @pl.when(i == NCB - 1)
        def _():
            edge[0].wait()

        norm_conv(b)
        mix_copy(b, own).start()

    phase("norm", 0, NCB, norm_step)

    loads[2].wait()
    loads[3].wait()
    edge[1].wait()
    lane = lax.broadcasted_iota(jnp.int32, (1, 128), 1)
    sign = jnp.where(lane % 64 < 32, -1.0, 1.0)
    docx[0:1, :] = jnp.where(place == 0, -1.0, dprev[7:8, :].astype(jnp.float32))
    docx[1:9, :] = doc[...].astype(jnp.float32)

    def table_step(b):
        rows = pl.ds(pl.multiple_of(b * WINDOW, WINDOW), WINDOW)
        cb = rope[2, pl.ds(place * NB + b, 1), :]
        sb = rope[3, pl.ds(place * NB + b, 1), :]
        cosv[rows, :] = rope[0] * cb - rope[1] * sb
        sinv[rows, :] = (rope[1] * cb + rope[0] * sb) * sign
        r = lax.broadcasted_iota(jnp.int32, (128, 128), 0)
        c = lax.broadcasted_iota(jnp.int32, (128, 128), 1)
        k0 = docx[pl.ds(b, 1), :]
        k1 = docx[pl.ds(b + 1, 1), :]
        mine = jnp.sum(jnp.where(r == c, k1, 0.0), axis=1, keepdims=True)
        bias[b, :, 0:128] = jnp.where(jnp.logical_and(c > r, k0 == mine), 0.0, NEG)
        bias[b, :, 128:256] = jnp.where(jnp.logical_and(c <= r, k1 == mine), 0.0, NEG)

    lax.fori_loop(0, NB, lambda b, carry: table_step(b), None)
    run(AFTER.get("table", {}).get(1, ()))

    def spread(dst, g, rows, v):
        low = lax.broadcasted_iota(jnp.int32, v.shape, 1) < 64
        turned = pltpu.roll(v, 64, 1)
        dst[g, 0, rows, :] = jnp.where(low, v, 0.0).astype(jnp.bfloat16)
        dst[g, 1, rows, :] = jnp.where(low, 0.0, turned).astype(jnp.bfloat16)
        dst[g, 2, rows, :] = jnp.where(low, turned, 0.0).astype(jnp.bfloat16)
        dst[g, 3, rows, :] = jnp.where(low, 0.0, v).astype(jnp.bfloat16)

    def product(g, rows, a, b):
        weights = jnp.concatenate([w[g, a], w[g, b]], axis=1)
        return jnp.dot(mixed[rows, :], weights, preferred_element_type=jnp.float32)

    def turn(v, rows):
        low = lax.broadcasted_iota(jnp.int32, (ROWS, 128), 1) % 64 < 32
        swapped = jnp.where(low, pltpu.roll(v, 96, 1), pltpu.roll(v, 32, 1))
        return v * cosv[rows, :] + swapped * sinv[rows, :]

    def project_kv(g, start):
        rows = pl.ds(start, ROWS)
        ext = pl.ds(pl.multiple_of(start + WINDOW, WINDOW), ROWS)
        p = product(g, rows, 0, CHUNKS)
        k = turn(p[:, 0:128], rows)
        v = p[:, 128:256]
        spread(kx, g, ext, k)
        spread(vx, g, ext, v)
        tail[start // ROWS, g, 0] = k[ROWS - WINDOW:].astype(jnp.bfloat16)
        tail[start // ROWS, g, 1] = v[ROWS - WINDOW:].astype(jnp.bfloat16)

    def project_q(g, j, start):
        rows = pl.ds(start, ROWS)
        p = product(g, rows, 1 + j, CHUNKS + 1 + j)
        for i in range(2):
            v = turn(p[:, i * 128:(i + 1) * 128], rows) * 0.125
            q[g, j, i, rows, :] = v.astype(jnp.bfloat16)

    def kv_phase(name, g, hooks=()):
        def body(i):
            project_kv(g, pl.multiple_of(((core + i) % 2) * ROWS, ROWS))

        phase(name, 0, 2, body, hooks)
        for i in range(2):
            kv_copy(g, i).start()

    def q_phase(name, g, low, high):
        phase(
            name, low, high,
            lambda i: project_q(g, i // 2, pl.multiple_of((i % 2) * ROWS, ROWS)),
        )

    def kv_copy(g, i):
        return remote(
            tail.at[1, g, i], halo.at[1 - g, i],
            kv_s.at[g, i], kv_r.at[1 - g, i], next_chip,
        )

    def attend(units):
        ones = lax.broadcasted_iota(jnp.int32, (512, 128), 0) // 256
        ones = ones == lax.broadcasted_iota(jnp.int32, (512, 128), 1) // 64
        ones = jnp.where(ones, 1.0, 0.0).astype(jnp.bfloat16)
        scores, weights = [], []
        for g, j, b in units:
            rows = pl.ds(pl.multiple_of(b * WINDOW, WINDOW), WINDOW)
            keys = pl.ds(pl.multiple_of(b * WINDOW, WINDOW), 2 * WINDOW)
            both = jnp.concatenate([q[g, j, 0, rows, :], q[g, j, 1, rows, :]], axis=0)
            k2 = jnp.concatenate([kx[g, 2 * j, keys, :], kx[g, 2 * j + 1, keys, :]], axis=0)
            scores.append(
                lax.dot_general(both, k2, (((1,), (1,)), ((), ())), preferred_element_type=jnp.float32)
            )
        for (g, j, b), s in zip(units, scores):
            extra = bias[b]
            extra = jnp.concatenate([extra, extra], axis=0)
            parts = []
            for i in range(2):
                half = s[:, i * 256:(i + 1) * 256] + extra
                e = jnp.exp(half - jnp.max(half, axis=1, keepdims=True))
                parts.append(e.astype(jnp.bfloat16))
            weights.append(jnp.concatenate(parts, axis=1))
        for (g, j, b), p in zip(units, weights):
            rows = pl.ds(pl.multiple_of(b * WINDOW, WINDOW), WINDOW)
            keys = pl.ds(pl.multiple_of(b * WINDOW, WINDOW), 2 * WINDOW)
            v2 = jnp.concatenate([vx[g, 2 * j, keys, :], vx[g, 2 * j + 1, keys, :]], axis=0)
            v2 = jnp.concatenate([v2, ones], axis=1)
            o = jnp.dot(p, v2, preferred_element_type=jnp.float32)
            o = (o[:, 0:128] / o[:, 128:256]).astype(jnp.bfloat16)
            att[g, j, rows, 0:128] = o[0:128]
            att[g, j, rows, 128:256] = o[128:256]

    def attend_phase(name, g, heads, low, high, sent):
        count = high - low
        rounds = count * len(heads) // UNITS if count > 1 else 1

        def body(i):
            each = 1 if count == 1 else UNITS // len(heads)
            blocks = [low + (i * each + n + (count // 2) * (1 - core)) % count for n in range(each)]
            attend([(g, j, b) for b in blocks for j in heads])

        def leave():
            for j in heads:
                att_copy(sent, j).start()

        phase(name, 0, rounds, body, {(rounds + 1) // 2: leave} if count != 7 else {4: leave})

    def halo_in(g):
        for i in range(2):
            copy = remote(
                halo.at[g, i], halo.at[g, i], kv_s.at[1 - g, i], kv_r.at[g, i], prev_chip
            )
            copy.wait_recv()
        spread(kx, g, pl.ds(0, WINDOW), halo[g, 0].astype(jnp.float32))
        spread(vx, g, pl.ds(0, WINDOW), halo[g, 1].astype(jnp.float32))

    def att_copy(k, j):
        g = k // 2
        start, count = ((128, ROWS - 128), (0, 128), (0, ROWS))[k]
        rows = pl.ds(pl.multiple_of(other + start, 128), count)
        dst = att2.at[g, j, pl.ds(start, count)]
        return remote(att.at[g, j, rows], dst, att_s.at[k, j], att_r.at[k, j], partner)

    def out_product(units, features, start, count):
        weights, heads = [], []
        rows = pl.ds(pl.multiple_of(own + start, 128), count)
        for g, j in units:
            weights += [w[g, 3 + j, features, :], w[g, CHUNKS + 3 + j, features, :]]
            weights += [w2[g, 2 * j, features, :], w2[g, 2 * j + 1, features, :]]
            heads += [att[g, j, rows, :], att2[g, j, start:start + count, :]]
        return lax.dot_general(
            jnp.concatenate(weights, axis=1), jnp.concatenate(heads, axis=1),
            (((1,), (1,)), ((), ())), preferred_element_type=jnp.float32,
        )

    def feature_rows(i):
        return pl.ds(pl.multiple_of(i * FC, 8), FC)

    near = ((0, 0), (0, 1))

    def out_near(i):
        rows = feature_rows(i)
        acc[rows, 128:ROWS] = out_product(near, rows, 128, ROWS - 128)

    def out_first(i):
        rows = feature_rows(i)
        acc[rows, 0:128] = out_product(near, rows, 0, 128)

    def out_last(i):
        rows = feature_rows(i)
        p = acc[rows, :] + out_product(((1, 0), (1, 1)), rows, 0, ROWS)
        outv[rows, :] = (flat[rows, :].astype(jnp.float32) + p).astype(jnp.bfloat16)

    for i in range(4, 10):
        loads[i].wait()
    def mixed_in():
        for b in range(NCB):
            mix_copy(b, other).wait_recv()
        for j in range(4):
            wo_copy(j).start()

    kv_phase("kv0", 0, {1: mixed_in})
    q_phase("q0", 0, 0, 4)
    attend_phase("own", 0, (0, 1), 1, NB, 0)
    for i in range(10, 14):
        loads[i].wait()
    for j in range(4):
        wo_copy(j).wait_recv()
    for j in range(2):
        att_copy(0, j).wait_recv()
    phase("of", 0, 4, out_near)
    kv_phase("kv1", 1)
    q_phase("q10", 1, 0, 2)
    halo_in(1)
    attend_phase("ar0", 1, (0,), 0, NB, 2)
    q_phase("q11", 1, 2, 4)
    halo_in(0)
    attend_phase("ao0", 0, (0, 1), 0, 1, 1)
    attend_phase("ar1", 1, (1,), 0, NB, 2)
    for j in range(2):
        att_copy(1, j).wait_recv()
    phase("of2", 0, 4, out_first)
    run(BEFORE.get("on", ()))
    far_arrived(3)
    att_copy(2, 0).wait_recv()
    run(BEFORE.get("ol", ()))
    far_arrived(4)
    att_copy(2, 1).wait_recv()
    lax.fori_loop(0, 4, lambda i, carry: out_last(i), None)

    for b in range(NCB):
        mix_copy(b, own).wait_send()
    for j in range(4):
        wo_copy(j).wait_send()
    for i in range(2):
        for g in range(2):
            kv_copy(g, i).wait_send()
        for k in range(3):
            att_copy(k, i).wait_send()
    for s in range(2):
        for c in range(CHUNKS):
            for kind in range(8):
                sending(s, c, kind).wait_send()
            if c >= 3:
                for k in range(4):
                    far_copy(s, c, k).wait_send()


def local(hidden_in, norm_gain, conv_weight, w_query, w_key, w_value, w_out, doc_ids):
    bf16, f32 = jnp.bfloat16, jnp.float32
    vmem, dma = pltpu.VMEM, pltpu.SemaphoreType.DMA
    scratch = [
        vmem((HALO + ROWS, D), bf16),
        vmem((D, ROWS), bf16),
        vmem((4, D), f32),
        vmem((CHIP, D), bf16),
        vmem((2, 2 * CHUNKS, D, 128), bf16),
        vmem((4, 128, 128), f32),
        vmem((CHIP, 128), f32),
        vmem((CHIP, 128), f32),
        vmem((8, 128), jnp.int32),
        vmem((8, 128), jnp.int32),
        vmem((16, 128), f32),
        vmem((NB, 128, 256), f32),
        vmem((2, 2, 2, CHIP, 128), bf16),
        vmem((2, 4, CHIP + WINDOW, 128), bf16),
        vmem((2, 4, CHIP + WINDOW, 128), bf16),
        vmem((2, 2, 2, WINDOW, 128), bf16),
        vmem((2, 2, WINDOW, 128), bf16),
        vmem((2, 2, CHIP, 256), bf16),
        vmem((2, 2, ROWS, 256), bf16),
        vmem((2, 4, D, 128), bf16),
        vmem((D, ROWS), f32),
        dma((14,)),
        dma((2, CHUNKS, 8)),
        dma((2, CHUNKS, 8)),
        dma((NCB,)),
        dma((NCB,)),
        dma((2,)),
        dma((2,)),
        dma((2, 2)),
        dma((2, 2)),
        dma((2, 3, 4)),
        dma((2, 3, 4)),
        dma((3, 2)),
        dma((3, 2)),
    ]
    hbm = pl.BlockSpec(memory_space=pl.ANY)
    out = pl.pallas_call(
        kernel,
        out_shape=pltpu.VMEM((D, ROWS), bf16),
        in_specs=[hbm, pl.BlockSpec(memory_space=pltpu.VMEM), *[hbm] * 7],
        out_specs=pl.BlockSpec(memory_space=pltpu.VMEM),
        scratch_shapes=scratch,
        compiler_params=pltpu.CompilerParams(
            collective_id=0, has_side_effects=True, vmem_limit_bytes=60 << 20
        ),
        name="attention_block",
    )(
        hidden_in.T, norm_gain, conv_weight, w_query, w_key, w_value, w_out.T,
        doc_ids.reshape(16, 128), jnp.asarray(rope_tables()),
    )
    return out.T


def solution(mesh):
    in_specs = (
        P(("dp", "seq", "tensor"), None),
        P(),
        P(),
        P(None, "tensor"),
        P(None, "tensor"),
        P(None, "tensor"),
        P("tensor", None),
        P(("dp", "seq")),
    )
    out_specs = P(("dp", "seq", "tensor"), None)
    return jax.shard_map(local, mesh=mesh, in_specs=in_specs, out_specs=out_specs, check_vma=False)
```
